256 devices in a mesh: wide: 32 (over z, y_hi, core), narrow: 8 (over x, y_lo).
Axes of the slice: x: 4, y: 4 (y_hi: 2, y_lo: 2; y = y_hi * 2 + y_lo), z: 8, core: 2. Of those that a mesh axis runs over, the one named last changes fastest.
Arguments:
- hidden: bfloat16 [65536, 8192], P(('wide', 'narrow')), may hold values from -24 to 24
- key_grad: bfloat16 [65536, 512], P(('wide', 'narrow')), may hold values from -6 to 6
- positions: int32 [65536], P(('wide', 'narrow')), may hold values from 0 to 4095
- weight_codes: bfloat16 [8192, 512], P('narrow'), may hold values from -127 to 127
- weight_scales: bfloat16 [8192, 2], P('narrow'), may hold values from 9.9658966e-05 to 0.0009994507
- master: float32 [8192, 512], P(('narrow', 'wide')), may hold values from -0.0625 to 0.0625
- moment: float32 [8192, 512], P(('narrow', 'wide')), may hold values from -6 to 6
- second: float32 [8192, 512], P(('narrow', 'wide')), may hold values from 0.5 to 4
Outputs:
- keys_out: bfloat16 [65536, 512], P(('wide', 'narrow'))
- hidden_grad: bfloat16 [65536, 8192], P(('wide', 'narrow'))
- gradient: float32 [8192, 512], P(('narrow', 'wide'))
- master_out: float32 [8192, 512], P(('narrow', 'wide'))
- moment_out: float32 [8192, 512], P(('narrow', 'wide'))
- second_out: float32 [8192, 512], P(('narrow', 'wide'))
- new_codes: bfloat16 [8192, 512], P('narrow')
- new_scales: bfloat16 [8192, 2], P('narrow')
The draws below stay inside these ranges and needn't reach their ends.
All inputs are finite; a program needn't handle non-finite values.
Results may differ from the reference program's by a relative error of at most 0.025.
Values may be sent and summed in bfloat16 or wider, within the bound.
A program may use at most 128 MiB of HBM per device.

```python
import math
import jax
import jax.numpy as jnp
from jax import lax

D = 8192
HEAD = 128
BLOCK = 256
TOK_DEV = 256
E = 512
BLOCKS = 2
TOKENS = 65536


def touch_ends(entries, rng, least, top_value):
    spot = [jax.random.randint(jax.random.fold_in(rng, axis), (), 0, length) for axis, length in enumerate(entries.shape)]
    longest = entries.shape.index(max(entries.shape))
    beside = spot[:longest] + [(spot[longest] + 1) % entries.shape[longest]] + spot[longest + 1:]
    return entries.at[tuple(spot)].set(least).at[tuple(beside)].set(top_value)


def with_spikes(result, rng, source, target, blocks, factor):
    owner, partner = [(jnp.arange(result.shape[dim]) // (result.shape[dim] // blocks)).reshape([-1 if axis == dim else 1 for axis in range(result.ndim)]) for dim in (source, target)]
    chosen = jax.random.permutation(rng, blocks)[partner]
    strong = (owner == chosen) | (owner == (partner + blocks // 2) % blocks)
    return jnp.where(strong, factor * result, result)


def block_scale(key, dims, pieces, low, high):
    level = 1.0
    for dim, parts in pieces:
        heights = jax.random.uniform(jax.random.fold_in(jax.random.fold_in(key, 6), dim), (parts,), jnp.float32, low / len(pieces), high / len(pieces))
        level = level * jnp.repeat(jnp.exp(heights), dims[dim] // parts).reshape((-1,) + (1,) * (len(dims) - 1 - dim))
    return level


def gaussian(stream_key, dims, scale, bound, split=(), held_as=jnp.bfloat16):
    entries = scale * jax.random.normal(stream_key, dims, jnp.float32)
    if split:
        entries = entries * block_scale(stream_key, dims, split, -0.22, 0.18)
    return jnp.clip(entries, -bound, bound).astype(held_as)


def heavy_noise(key, dims, deviation, reach, split, heavy, kind=jnp.bfloat16):
    drawn = deviation * jax.random.normal(key, dims, jnp.float32)
    if split:
        drawn = drawn * block_scale(key, dims, split, -0.22, 0.18)
    return jnp.clip(with_spikes(drawn, jax.random.fold_in(key, 3), *heavy), -reach, reach).astype(kind)


def setup_inputs(seed: int = 0) -> dict:
    streams_of = jax.random.split(jax.random.key(seed), 9)
    return {
        "hidden": heavy_noise(streams_of[0], (TOKENS, D), 1.0, 24.0, ((0, 256),), (0, 1, 256, 6.0)),
        "key_grad": gaussian(streams_of[1], (TOKENS, E), 1.0, 6.0, ((0, 256),)),
        "positions": touch_ends(jax.random.randint(streams_of[2], (TOKENS,), 0, 4096), jax.random.fold_in(streams_of[2], 1), 0, 4095).astype(jnp.int32),
        "weight_codes": jnp.clip(jax.random.uniform(streams_of[3], (D, E), jnp.float32, -127.0, 127.0) * block_scale(streams_of[3], (D, E), ((0, 8),), -0.4, 0.0), -127.0, 127.0).astype(jnp.bfloat16),
        "weight_scales": jnp.clip(jnp.exp(math.log(0.0009994507) - 2.3054518 * jax.random.uniform(streams_of[4], (D, BLOCKS), jnp.float32) ** block_scale(streams_of[4], (D, BLOCKS), ((0, 8),), -0.2, 0.2)), 9.965896606445312e-05, 0.0009994507).astype(jnp.bfloat16),
        "master": gaussian(streams_of[5], (D, E), D ** -0.5, 0.0625, ((0, 256),), jnp.float32),
        "moment": gaussian(streams_of[6], (D, E), 1.0, 6.0, ((0, 256),), jnp.float32),
        "second": jnp.clip(jnp.exp(math.log(4.0) - 2.0794415 * jax.random.uniform(streams_of[7], (D, E), jnp.float32) ** block_scale(streams_of[7], (D, E), ((0, 256),), -0.2, 0.2)), 0.5, 4.0),
    }


ROPE_BASE = 1000000.0
LEARN_RATE = 0.002
FIRST_DECAY = 0.9
SECOND_DECAY = 0.95
FIRST_FIX = 0.9999734386011124
SECOND_FIX = 0.994079470779666
ADAM_EPSILON = 1e-08
SCALE_EPSILON = 1e-06
CODE_RANGE = 127.0

def dequantize(weight_codes, weight_scales):
    height, width = weight_codes.shape
    blocks = weight_scales.shape[1]
    grouped = weight_codes.astype(jnp.float32).reshape(height, blocks, width // blocks)
    grouped = grouped * weight_scales.astype(jnp.float32)[:, :, None]
    return grouped.reshape(height, width).astype(jnp.bfloat16)

def rotation(positions, head_size):
    half_size = head_size // 2
    powers = jnp.arange(half_size, dtype=jnp.float32) * (-2.0 / head_size)
    frequency = jnp.power(jnp.float32(ROPE_BASE), powers)
    angles = positions.astype(jnp.float32)[:, None] * frequency[None, :]
    cosine = jnp.cos(angles)
    sines = jnp.sin(angles)
    return (jnp.concatenate([cosine, cosine], 1), jnp.concatenate([sines, sines], 1))

def turn_half(values):
    half_size = values.shape[-1] // 2
    return jnp.concatenate([-values[..., half_size:], values[..., :half_size]], -1)

def apply_rotation(values, cosine, sines, head_size):
    count, width = values.shape
    heads = values.reshape(count, width // head_size, head_size)
    turned = heads * cosine[:, None, :] + turn_half(heads) * sines[:, None, :]
    return turned.reshape(count, width)

def undo_rotation(values, cosine, sines, head_size):
    count, width = values.shape
    heads = values.reshape(count, width // head_size, head_size)
    scaled = heads * sines[:, None, :]
    reverted = heads * cosine[:, None, :] - turn_half(scaled)
    return reverted.reshape(count, width)

def adam_update(gradient, master, moment, second):
    moment_out = FIRST_DECAY * moment + (1.0 - FIRST_DECAY) * gradient
    second_out = SECOND_DECAY * second + (1.0 - SECOND_DECAY) * gradient * gradient
    step_size = moment_out / FIRST_FIX / (jnp.sqrt(second_out / SECOND_FIX) + ADAM_EPSILON)
    master_out = master - LEARN_RATE * step_size
    return (master_out, moment_out, second_out)

def requantize(master_out, block_width):
    height, width = master_out.shape
    grouped = master_out.reshape(height, width // block_width, block_width)
    peak = lax.optimization_barrier(jnp.max(jnp.abs(grouped), axis=2))
    new_scales = ((peak + SCALE_EPSILON) / CODE_RANGE).astype(jnp.bfloat16)
    divisor = lax.optimization_barrier(new_scales).astype(jnp.float32)
    new_codes = (grouped / divisor[:, :, None]).reshape(height, width).astype(jnp.bfloat16)
    return (new_codes, new_scales)

def reference(hidden, key_grad, positions, weight_codes, weight_scales, master, moment, second):
    weight = dequantize(weight_codes, weight_scales)
    cosine, sines = rotation(positions, HEAD)
    raw_keys = jnp.dot(hidden, weight, preferred_element_type=jnp.float32)
    keys_out = apply_rotation(raw_keys, cosine, sines, HEAD).astype(jnp.bfloat16)
    back_grad = undo_rotation(key_grad.astype(jnp.float32), cosine, sines, HEAD).astype(jnp.bfloat16)
    hidden_grad = lax.dot_general(back_grad, weight, (((1,), (1,)), ((), ())), preferred_element_type=jnp.float32).astype(jnp.bfloat16)
    block_count = TOKENS // TOK_DEV

    def add_block(running, inputs_pair):
        block_rows, block_back = inputs_pair
        partial_value = lax.dot_general(block_rows, block_back, (((0,), (0,)), ((), ())), preferred_element_type=jnp.float32).astype(jnp.bfloat16)
        partial_value = lax.optimization_barrier(partial_value)
        return (running + partial_value.astype(jnp.float32), None)
    summed, _ = lax.scan(add_block, jnp.zeros((D, E), jnp.float32), (hidden.reshape(block_count, TOK_DEV, D), back_grad.reshape(block_count, TOK_DEV, E)))
    gradient = summed / jnp.float32(block_count)
    master_out, moment_out, second_out = adam_update(gradient, master, moment, second)
    new_codes, new_scales = requantize(master_out, BLOCK)
    return (keys_out, hidden_grad, gradient, master_out, moment_out, second_out, new_codes, new_scales)
```

```python
import jax
import jax.numpy as jnp
from jax import lax
from jax.experimental import pallas as pl
from jax.experimental.pallas import tpu as pltpu
from jax.sharding import PartitionSpec as P

HEAD = 128
ROPE_BASE = 1000000.0
LEARN_RATE = 0.002
FIRST_DECAY = 0.9
SECOND_DECAY = 0.95
FIRST_FIX = 0.9999734386011124
SECOND_FIX = 0.994079470779666
ADAM_EPSILON = 1e-08
SCALE_EPSILON = 1e-06
CODE_RANGE = 127.0

MESH = pl.DeviceIdType.MESH
F32 = jnp.float32
BF16 = jnp.bfloat16
ZN = 8
STEPS = ZN - 1
LAG = 3


def device(z, y, x, core):
    return (z * 4 + lax.div(y, 2) * 2 + core, x * 2 + lax.rem(y, 2))


def dot_rows(a, b):
    return lax.dot_general(a, b, (((0,), (0,)), ((), ())), preferred_element_type=F32)


def exchange_kernel(
    hid_hbm, key_grad, cosine, sines, codes, scales, master, moment, second,
    w_hbm, back_out, keys_out, grad_out, master_out, moment_out, second_out, cg_hbm,
    hid, hidp, backp, wg, pbuf, sendbuf, recvbuf, zsum, a2a, cg, acc,
    hid_sem, w_sem, cg_sem, hsend, hrecv, bsend, brecv, wsend, wrecv,
    zsend, zrecv, asend, arecv, gsend, grecv, dsend, drecv,
):
    wide = lax.axis_index("wide")
    narrow = lax.axis_index("narrow")
    z, yh, c = lax.div(wide, 4), lax.rem(lax.div(wide, 2), 2), lax.rem(wide, 2)
    x, yl = lax.div(narrow, 2), lax.rem(narrow, 2)
    y = yh * 2 + yl
    oc = 1 - c
    partner = device(z, y, x, oc)
    xs = {d: lax.rem(x + d + 4, 4) for d in (-1, 1, 2)}
    xs[0] = x
    ys = {d: lax.rem(y + d + 4, 4) for d in (-1, 1)}

    load = pltpu.make_async_copy(hid_hbm, hid, hid_sem)
    load.start()

    def send_hidden(xd):
        cols = pl.ds(pl.multiple_of((xd * 2 + oc) * 1024, 1024), 1024)
        return pltpu.make_async_remote_copy(
            hid_hbm.at[:, cols], hidp.at[xd], hsend, hrecv.at[xd], partner, MESH
        )

    for xd in range(4):
        send_hidden(xd).start()

    lane = lax.broadcasted_iota(jnp.int32, (256, HEAD), 1)
    cos = cosine[...]
    sin = jnp.where(lane < HEAD // 2, -sines[...], sines[...])
    for h in range(4):
        s = slice(h * HEAD, (h + 1) * HEAD)
        v = key_grad[:, s].astype(F32)
        back_out[:, s] = (v * cos - pltpu.roll(v, HEAD // 2, 1) * sin).astype(BF16)
    send_back = pltpu.make_async_remote_copy(back_out, backp, bsend, brecv, partner, MESH)
    send_back.start()

    pick = (
        lax.broadcasted_iota(jnp.int32, (2, 512), 1) // 256
        == lax.broadcasted_iota(jnp.int32, (2, 512), 0)
    ).astype(BF16)

    @pl.loop(0, 8)
    def _(i):
        rows = pl.ds(pl.multiple_of(i * 128, 128), 128)
        factor = dot_rows(scales[:, rows], pick)
        wg[narrow, rows, :] = (codes[rows, :].astype(F32) * factor).astype(BF16)

    def chunk(xb, lo, half, q):
        return wg.at[xb * 2 + lo, pl.ds(pl.multiple_of(half * 512 + q * 256, 256), 256)]

    def w_copy(xb, lo, half, q, target):
        ref = chunk(xb, lo, half, q)
        sem = wrecv.at[xb * 2 + lo, half, q]
        return pltpu.make_async_remote_copy(ref, ref, wsend, sem, target, MESH)

    def w_wait(xb, lo, half, q):
        w_copy(xb, lo, half, q, partner).wait_recv()

    def to_x(xb, q, d):
        w_copy(xb, yl, c, q, device(z, y, xs[d], c)).start()

    def to_y(xb, q):
        w_copy(xb, yl, c, q, device(z, ys[1 - 2 * q], x, c)).start()

    def to_partner(xb, lo, q):
        w_copy(xb, lo, c, q, partner).start()

    for q in range(2):
        to_x(x, q, 1)
        to_x(x, q, -1)
        to_y(x, q)

    load.wait()

    def keys_of(xb, lo, first=False):
        block = xb * 2 + lo
        if not first:
            w_wait(xb, lo, oc, 0)
            w_wait(xb, lo, oc, 1)
        pltpu.make_async_copy(wg.at[block], w_hbm.at[block], w_sem).start()
        cols = pl.ds(pl.multiple_of(block * 1024, 1024), 1024)
        term = jnp.dot(hid[:, cols], wg[block], preferred_element_type=F32)
        acc[...] = term if first else acc[...] + term

    def partials(p, step):
        for xd in range(4):
            way = 1 if xd < 2 else -1
            at = lax.rem(z - way * (step + 1) + 2 * ZN, ZN)
            own = pl.ds(pl.multiple_of((xd * 2 + c) * 1024 + at * 128, 128), 128)
            other = pl.ds(pl.multiple_of(at * 128, 128), 128)
            cols = slice(p * 256, (p + 1) * 256)
            pbuf[p, xd] = dot_rows(hid[:, own], back_out[:, cols]) + dot_rows(
                hidp[xd, :, other], backp[:, cols]
            )

    def z_copy(p, xd, step):
        way = 1 if xd < 2 else -1
        to = device(lax.rem(z + way + ZN, ZN), y, x, c)
        return pltpu.make_async_remote_copy(
            sendbuf.at[p, xd, step], recvbuf.at[p, xd, step],
            zsend, zrecv.at[p, xd, step], to, MESH,
        )

    def z_step(p, step):
        for xd in range(4):
            @pl.when(step > 0)
            def _():
                z_copy(p, xd, step - 1).wait_recv()
                pbuf[p, xd] += recvbuf[p, xd, step - 1].astype(F32)

            sendbuf[p, xd, step] = pbuf[p, xd].astype(BF16)
            z_copy(p, xd, step).start()
        partials(p, step + 1)

    def plane_copy(p, i):
        xd, yhd, cd = lax.div(i, 4), lax.rem(lax.div(i, 2), 2), lax.rem(i, 2)
        rows = pl.ds(pl.multiple_of(yhd * 64 + cd * 32, 32), 32)
        src, dst = zsum.at[p, xd, rows], a2a.at[p, x * 4 + y]
        mine = (xd == x) & (yl == c) & (yhd == yh) & (cd == c)
        remote = pltpu.make_async_remote_copy(
            src, dst, asend.at[p], arecv.at[p], device(z, yhd * 2 + c, xd, cd), MESH
        )
        return mine, remote, pltpu.make_async_copy(src, dst, arecv.at[p])

    def to_plane(p):
        for xd in range(4):
            z_copy(p, xd, STEPS - 1).wait_recv()
            zsum[p, xd] = (pbuf[p, xd] + recvbuf[p, xd, STEPS - 1].astype(F32)).astype(BF16)

        @pl.loop(0, 16)
        def _(i):
            mine, remote, local = plane_copy(p, i)

            @pl.when(mine)
            def _():
                local.start()

            @pl.when(jnp.logical_not(mine))
            def _():
                remote.start()

    def span(p):
        return slice(0, 256) if p == 0 else slice(256, 640)

    def code_copy(p, i):
        zd, yhd = lax.div(i, 2), lax.rem(i, 2)
        ref = cg.at[z, yh, c, :, span(p)]
        mine = (zd == z) & (yhd == yh)
        return mine, pltpu.make_async_remote_copy(
            ref, ref, gsend.at[p], grecv.at[p], device(zd, yhd * 2 + yl, x, c), MESH
        )

    def update(p):
        pltpu.make_async_copy(a2a.at[p], a2a.at[p], arecv.at[p]).wait()
        total = a2a[p, 0].astype(F32)
        for i in range(1, 16):
            total = total + a2a[p, i].astype(F32)
        cols = slice(p * 256, (p + 1) * 256)
        gradient = total / 256.0
        moment_new = FIRST_DECAY * moment[:, cols] + (1.0 - FIRST_DECAY) * gradient
        second_new = SECOND_DECAY * second[:, cols] + (1.0 - SECOND_DECAY) * gradient * gradient
        step_size = moment_new / FIRST_FIX / (jnp.sqrt(second_new / SECOND_FIX) + ADAM_EPSILON)
        master_new = master[:, cols] - LEARN_RATE * step_size
        grad_out[:, cols] = gradient
        moment_out[:, cols] = moment_new
        second_out[:, cols] = second_new
        master_out[:, cols] = master_new
        peak = jnp.max(jnp.abs(master_new), axis=1, keepdims=True)
        scale = ((peak + SCALE_EPSILON) / CODE_RANGE).astype(BF16).astype(F32)
        cg[z, yh, c, :, cols] = (master_new / scale).astype(BF16)
        spread = jnp.broadcast_to(scale, (32, HEAD))
        if p == 1:
            at = lax.broadcasted_iota(jnp.int32, (32, HEAD), 1)
            spread = jnp.where(at == 0, cg[z, yh, c, :, 512:640].astype(F32), spread)
        cg[z, yh, c, :, 512:640] = spread.astype(BF16)

        @pl.loop(0, 16)
        def _(i):
            mine, remote = code_copy(p, i)

            @pl.when(jnp.logical_not(mine))
            def _():
                remote.start()

    def fifteen(p, sem):
        same = a2a.at[0, pl.ds(0, 15)] if p == 0 else hid.at[0:32, 0 : 15 * 384]
        pltpu.make_async_copy(same, same, sem).wait()

    def pass_copy(p):
        ref = cg.at[:, :, c, :, span(p)]
        return pltpu.make_async_remote_copy(
            ref, ref, dsend.at[p], drecv.at[p], partner, MESH
        )

    for xd in range(4):
        send_hidden(xd).wait_recv()
    send_back.wait_recv()
    partials(0, 0)

    @pl.loop(0, STEPS + LAG)
    def _(t):
        @pl.when(t < STEPS)
        def _():
            z_step(0, t)

        @pl.when(t == LAG - 1)
        def _():
            partials(1, 0)
            keys_of(x, yl, True)

        @pl.when(t >= LAG)
        def _():
            z_step(1, t - LAG)

        @pl.when(t == 2)
        def _():
            w_wait(xs[-1], yl, c, 0)
            to_x(xs[-1], 0, 1)
            to_y(xs[-1], 0)
            to_partner(xs[-1], yl, 0)
            w_wait(xs[1], yl, c, 0)
            to_y(xs[1], 0)
            to_partner(xs[1], yl, 0)
            for q in range(2):
                w_wait(x, 1 - yl, c, q)
                to_partner(x, 1 - yl, q)

        @pl.when(t == 3)
        def _():
            w_wait(xs[1], yl, c, 1)
            to_x(xs[1], 1, -1)
            to_y(xs[1], 1)
            to_partner(xs[1], yl, 1)
            w_wait(xs[-1], yl, c, 1)
            to_y(xs[-1], 1)
            to_partner(xs[-1], yl, 1)
            keys_of(x, 1 - yl)

        @pl.when(t == 4)
        def _():
            for q in range(2):
                w_wait(xs[2], yl, c, q)
                to_y(xs[2], q)
                to_partner(xs[2], yl, q)
            for d in (-1, 1):
                w_wait(xs[d], 1 - yl, c, 0)
                to_partner(xs[d], 1 - yl, 0)
            for d in (-1, 1):
                keys_of(xs[d], yl)

        @pl.when(t == 5)
        def _():
            for d in (-1, 1):
                w_wait(xs[d], 1 - yl, c, 1)
                to_partner(xs[d], 1 - yl, 1)
            keys_of(xs[2], yl)

        @pl.when(t == 6)
        def _():
            for q in range(2):
                w_wait(xs[2], 1 - yl, c, q)
                to_partner(xs[2], 1 - yl, q)
            for d in (-1, 1):
                keys_of(xs[d], 1 - yl)
            to_plane(0)

        @pl.when(t == 7)
        def _():
            keys_of(xs[2], 1 - yl)

        @pl.when(t == 8)
        def _():
            update(0)

    to_plane(1)
    for h in range(4):
        s = slice(h * HEAD, (h + 1) * HEAD)
        v = acc[:, s]
        keys_out[:, s] = (v * cos + pltpu.roll(v, HEAD // 2, 1) * sin).astype(BF16)
    fifteen(0, grecv.at[0])
    pass_copy(0).start()
    update(1)
    fifteen(1, grecv.at[1])
    pass_copy(1).start()

    pltpu.make_async_copy(hidp, hidp, hsend).wait()
    send_back.wait_send()
    pltpu.make_async_copy(wg.at[pl.ds(0, 7)], wg.at[pl.ds(0, 7)], wsend).wait()
    pltpu.make_async_copy(sendbuf, sendbuf, zsend).wait()
    for p in range(2):
        @pl.when(yl == c)
        def _():
            part = a2a.at[p, pl.ds(0, 15)]
            pltpu.make_async_copy(part, part, asend.at[p]).wait()

        @pl.when(yl != c)
        def _():
            pltpu.make_async_copy(a2a.at[p], a2a.at[p], asend.at[p]).wait()

        fifteen(p, gsend.at[p])
        pass_copy(p).wait()
    pltpu.make_async_copy(wg, w_hbm, w_sem).wait()
    last = pltpu.make_async_copy(cg, cg_hbm, cg_sem)
    last.start()
    last.wait()


def exchange(hidden, key_grad, cosine, sines, codes, scales, master, moment, second):
    vmem = pl.BlockSpec(memory_space=pltpu.VMEM)
    anywhere = pl.BlockSpec(memory_space=pl.ANY)
    dma = pltpu.SemaphoreType.DMA
    state = jax.ShapeDtypeStruct((32, 512), F32)
    return pl.pallas_call(
        exchange_kernel,
        out_shape=(
            jax.ShapeDtypeStruct((8, 1024, 512), BF16),
            jax.ShapeDtypeStruct((256, 512), BF16),
            jax.ShapeDtypeStruct((256, 512), BF16),
            state, state, state, state,
            jax.ShapeDtypeStruct((8, 2, 2, 32, 640), BF16),
        ),
        in_specs=[anywhere] + [vmem] * 8,
        out_specs=(anywhere,) + (vmem,) * 6 + (anywhere,),
        scratch_shapes=[
            pltpu.VMEM((256, 8192), BF16),
            pltpu.VMEM((4, 256, 1024), BF16),
            pltpu.VMEM((256, 512), BF16),
            pltpu.VMEM((8, 1024, 512), BF16),
            pltpu.VMEM((2, 4, 128, 256), F32),
            pltpu.VMEM((2, 4, STEPS, 128, 256), BF16),
            pltpu.VMEM((2, 4, STEPS, 128, 256), BF16),
            pltpu.VMEM((2, 4, 128, 256), BF16),
            pltpu.VMEM((2, 16, 32, 256), BF16),
            pltpu.VMEM((8, 2, 2, 32, 640), BF16),
            pltpu.VMEM((256, 512), F32),
            dma, dma, dma,
            dma, dma((4,)), dma, dma, dma, dma((8, 2, 2)),
            dma, dma((2, 4, STEPS)),
            dma((2,)), dma((2,)), dma((2,)), dma((2,)), dma((2,)), dma((2,)),
        ],
        compiler_params=pltpu.CompilerParams(
            has_side_effects=True, vmem_limit_bytes=60 * 1024 * 1024
        ),
    )(hidden, key_grad, cosine, sines, codes, scales, master, moment, second)


def finish_kernel(
    w, back, keys, grad, master, moment, second, cg,
    hidden_grad, keys_out, grad_out, master_out, moment_out, second_out, codes_out, scales_out,
):
    hidden_grad[...] = lax.dot_general(
        back[...], w[0], (((1,), (1,)), ((), ())), preferred_element_type=F32
    ).astype(BF16)

    @pl.when(pl.program_id(0) == 0)
    def _():
        keys_out[...] = keys[...]
        grad_out[...] = grad[...]
        master_out[...] = master[...]
        moment_out[...] = moment[...]
        second_out[...] = second[...]
        codes_out[...] = cg[:, 0:512]
        scales_out[...] = cg[:, 512:640].astype(F32).T[0:2, :].astype(BF16)


def finish(w, back, keys, grad, master, moment, second, cg):
    def whole(*shape):
        return pl.BlockSpec(shape, lambda i: (0,) * len(shape))

    state = jax.ShapeDtypeStruct((32, 512), F32)
    return pl.pallas_call(
        finish_kernel,
        grid=(8,),
        out_shape=(
            jax.ShapeDtypeStruct((256, 8192), BF16),
            jax.ShapeDtypeStruct((256, 512), BF16),
            state, state, state, state,
            jax.ShapeDtypeStruct((1024, 512), BF16),
            jax.ShapeDtypeStruct((2, 1024), BF16),
        ),
        in_specs=[
            pl.BlockSpec((1, 1024, 512), lambda i: (i, 0, 0)),
            whole(256, 512), whole(256, 512),
            whole(32, 512), whole(32, 512), whole(32, 512), whole(32, 512),
            whole(1024, 640),
        ],
        out_specs=(
            pl.BlockSpec((256, 1024), lambda i: (0, i)),
            whole(256, 512),
            whole(32, 512), whole(32, 512), whole(32, 512), whole(32, 512),
            whole(1024, 512), whole(2, 1024),
        ),
    )(w, back, keys, grad, master, moment, second, cg)


def rotation(positions):
    half_size = HEAD // 2
    powers = jnp.arange(half_size, dtype=F32) * (-2.0 / HEAD)
    frequency = jnp.power(F32(ROPE_BASE), powers)
    both = jnp.concatenate([frequency, frequency])
    angles = positions.astype(F32)[:, None] * both[None, :]
    return jnp.cos(angles), jnp.sin(angles)


def shards(hidden, key_grad, positions, weight_codes, weight_scales, master, moment, second):
    cosine, sines = rotation(positions)
    w, back, keys, grad, master_out, moment_out, second_out, cg = exchange(
        hidden, key_grad, cosine, sines, weight_codes, weight_scales.T, master, moment, second
    )
    hidden_grad, keys, grad, master_out, moment_out, second_out, codes, scales = finish(
        w, back, keys, grad, master_out, moment_out, second_out, cg.reshape(1024, 640)
    )
    return (keys, hidden_grad, grad, master_out, moment_out, second_out, codes, scales.T)


def solution(mesh):
    in_specs = (
        P(("wide", "narrow"), None),
        P(("wide", "narrow"), None),
        P(("wide", "narrow")),
        P("narrow", None),
        P("narrow", None),
        P(("narrow", "wide"), None),
        P(("narrow", "wide"), None),
        P(("narrow", "wide"), None),
    )
    out_specs = (
        P(("wide", "narrow"), None),
        P(("wide", "narrow"), None),
        P(("narrow", "wide"), None),
        P(("narrow", "wide"), None),
        P(("narrow", "wide"), None),
        P(("narrow", "wide"), None),
        P("narrow", None),
        P("narrow", None),
    )
    return jax.shard_map(shards, mesh=mesh, in_specs=in_specs, out_specs=out_specs, check_vma=False)
```

```python
import jax
import jax.numpy as jnp
from jax import lax
from jax.experimental import pallas as pl
from jax.experimental.pallas import tpu as pltpu
from jax.sharding import PartitionSpec as P

HEAD = 128
ROPE_BASE = 1000000.0
LEARN_RATE = 0.002
FIRST_DECAY = 0.9
SECOND_DECAY = 0.95
FIRST_FIX = 0.9999734386011124
SECOND_FIX = 0.994079470779666
ADAM_EPSILON = 1e-08
SCALE_EPSILON = 1e-06
CODE_RANGE = 127.0

MESH = pl.DeviceIdType.MESH
F32 = jnp.float32
BF16 = jnp.bfloat16
ZN = 8
STEPS = ZN - 1
LAG = 3


def device(z, y, x, core):
    return (z * 4 + lax.div(y, 2) * 2 + core, x * 2 + lax.rem(y, 2))


def dot_rows(a, b):
    return lax.dot_general(a, b, (((0,), (0,)), ((), ())), preferred_element_type=F32)


def exchange_kernel(
    hid_hbm, key_grad_hbm, positions, frequency, codes_hbm, scales, master_hbm, moment_hbm,
    second_hbm,
    hg_hbm, keys_hbm, grad_hbm, master_out_hbm, moment_out_hbm, second_out_hbm, cg_hbm,
    hid, hidp, back_out, backp, wg, hg, pbuf, sendbuf, recvbuf, zsum, a2a, cg, acc,
    key_grad, codes, keys_out, state,
    in_sem, hg_sem, cg_sem, out_sem, hsend, hrecv, bsend, brecv, wsend, wrecv,
    zsend, zrecv, asend, arecv, gsend, grecv, ysend, yrecv, dsend, drecv,
):
    master, moment, second, grad_out, master_out, moment_out, second_out = (
        state.at[i] for i in range(7)
    )
    wide = lax.axis_index("wide")
    narrow = lax.axis_index("narrow")
    z, yh, c = lax.div(wide, 4), lax.rem(lax.div(wide, 2), 2), lax.rem(wide, 2)
    x, yl = lax.div(narrow, 2), lax.rem(narrow, 2)
    y = yh * 2 + yl
    oc = 1 - c
    partner = device(z, y, x, oc)
    xs = {d: lax.rem(x + d + 4, 4) for d in (-1, 1, 2)}
    xs[0] = x
    ys = {d: lax.rem(y + d + 4, 4) for d in (-1, 1)}

    loads = [
        pltpu.make_async_copy(src, dst, in_sem.at[i])
        for i, (src, dst) in enumerate((
            (key_grad_hbm, key_grad), (codes_hbm, codes), (hid_hbm, hid),
            (master_hbm, master), (moment_hbm, moment), (second_hbm, second),
        ))
    ]
    for load in loads:
        load.start()

    barrier = pltpu.get_barrier_semaphore()

    @pl.loop(0, 32)
    def _(i):
        to = device(z, lax.rem(lax.div(i, 2), 4), lax.div(i, 8), lax.rem(i, 2))

        @pl.when((to[0] != wide) | (to[1] != narrow))
        def _():
            pl.semaphore_signal(barrier, inc=1, device_id=to, device_id_type=MESH)

    @pl.loop(0, 16)
    def _(i):
        @pl.when(lax.div(i, 2) != z)
        def _():
            to = device(lax.div(i, 2), lax.rem(i, 2) * 2 + yl, x, c)
            pl.semaphore_signal(barrier, inc=1, device_id=to, device_id_type=MESH)

    def send_hidden(xd):
        cols = pl.ds(pl.multiple_of((xd * 2 + oc) * 1024, 1024), 1024)
        return pltpu.make_async_remote_copy(
            hid_hbm.at[:, cols], hidp.at[xd], hsend, hrecv.at[xd], partner, MESH
        )

    place = jnp.concatenate(
        [jnp.broadcast_to(positions[i : i + 1, :].astype(F32), (128, 128)).T for i in range(2)], 0
    )
    angle = place * frequency[...]
    cos = jnp.cos(angle)
    sin = jnp.sin(angle)
    lane = lax.broadcasted_iota(jnp.int32, (256, HEAD), 1)
    sin = jnp.where(lane < HEAD // 2, -sin, sin)
    loads[0].wait()
    for h in range(4):
        s = slice(h * HEAD, (h + 1) * HEAD)
        v = key_grad[:, s].astype(F32)
        back_out[:, s] = (v * cos - pltpu.roll(v, HEAD // 2, 1) * sin).astype(BF16)
    send_back = pltpu.make_async_remote_copy(back_out, backp, bsend, brecv, partner, MESH)

    pick = (
        lax.broadcasted_iota(jnp.int32, (2, 512), 1) // 256
        == lax.broadcasted_iota(jnp.int32, (2, 512), 0)
    ).astype(BF16)

    loads[1].wait()

    @pl.loop(0, 8)
    def _(i):
        rows = pl.ds(pl.multiple_of(i * 128, 128), 128)
        factor = dot_rows(scales[:, rows], pick)
        wg[narrow, rows, :] = (codes[rows, :].astype(F32) * factor).astype(BF16)

    def chunk(xb, lo, half, q):
        return wg.at[xb * 2 + lo, pl.ds(pl.multiple_of(half * 512 + q * 256, 256), 256)]

    def w_copy(xb, lo, half, q, target):
        ref = chunk(xb, lo, half, q)
        sem = wrecv.at[xb * 2 + lo, half, q]
        return pltpu.make_async_remote_copy(ref, ref, wsend, sem, target, MESH)

    def w_wait(xb, lo, half, q):
        w_copy(xb, lo, half, q, partner).wait_recv()

    def to_x(xb, q, d):
        w_copy(xb, yl, c, q, device(z, y, xs[d], c)).start()

    def to_y(xb, q):
        w_copy(xb, yl, c, q, device(z, ys[1 - 2 * q], x, c)).start()

    def to_partner(xb, lo, q):
        w_copy(xb, lo, c, q, partner).start()

    pl.semaphore_wait(barrier, 45)
    for xd in range(4):
        send_hidden(xd).start()
    send_back.start()
    for q in range(2):
        to_x(x, q, 1)
        to_x(x, q, -1)
        to_y(x, q)

    for load in loads[2:]:
        load.wait()

    def hg_copy(block):
        cols = pl.ds(pl.multiple_of(block * 1024, 1024), 1024)
        return pltpu.make_async_copy(hg.at[:, cols], hg_hbm.at[:, cols], hg_sem)

    def use_block(xb, lo, first=False):
        block = xb * 2 + lo
        if first:
            acc[...] = jnp.zeros_like(acc)
        else:
            w_wait(xb, lo, oc, 0)
            w_wait(xb, lo, oc, 1)

        @pl.loop(0, 4)
        def _(i):
            cols = pl.ds(pl.multiple_of(block * 1024 + i * 256, 256), 256)
            w = wg[block, pl.ds(pl.multiple_of(i * 256, 256), 256), :]
            acc[...] += jnp.dot(hid[:, cols], w, preferred_element_type=F32)
            hg[:, cols] = lax.dot_general(
                back_out[...], w, (((1,), (1,)), ((), ())), preferred_element_type=F32
            ).astype(BF16)

        hg_copy(block).start()

    def partials(p, step):
        for xd in range(4):
            way = 1 if xd < 2 else -1
            at = lax.rem(z - way * (step + 1) + 2 * ZN, ZN)
            own = pl.ds(pl.multiple_of((xd * 2 + c) * 1024 + at * 128, 128), 128)
            other = pl.ds(pl.multiple_of(at * 128, 128), 128)
            cols = slice(p * 256, (p + 1) * 256)
            pbuf[p, xd] = dot_rows(hid[:, own], back_out[:, cols]) + dot_rows(
                hidp[xd, :, other], backp[:, cols]
            )

    def z_copy(p, xd, half, step):
        way = 1 if xd < 2 else -1
        to = device(lax.rem(z + way + ZN, ZN), y, x, c)
        rows = slice(half * 64, half * 64 + 64)
        return pltpu.make_async_remote_copy(
            sendbuf.at[p, xd, step, rows], recvbuf.at[p, xd, step, rows],
            zsend, zrecv.at[p, xd, half, step], to, MESH,
        )

    def z_step(p, step):
        for half in range(2):
            rows = slice(half * 64, half * 64 + 64)
            for xd in (0, 2, 1, 3):
                @pl.when(step > 0)
                def _():
                    z_copy(p, xd, half, step - 1).wait_recv()
                    pbuf[p, xd, rows] += recvbuf[p, xd, step - 1, rows].astype(F32)

                sendbuf[p, xd, step, rows] = pbuf[p, xd, rows].astype(BF16)
                z_copy(p, xd, half, step).start()
        partials(p, step + 1)

    def plane_copy(p, i):
        xd, yhd, cd = lax.div(i, 4), lax.rem(lax.div(i, 2), 2), lax.rem(i, 2)
        rows = pl.ds(pl.multiple_of(yhd * 64 + cd * 32, 32), 32)
        src, dst = zsum.at[p, xd, rows], a2a.at[p, x * 4 + y]
        mine = (xd == x) & (yl == c) & (yhd == yh) & (cd == c)
        remote = pltpu.make_async_remote_copy(
            src, dst, asend.at[p], arecv.at[p], device(z, yhd * 2 + c, xd, cd), MESH
        )
        return mine, remote, pltpu.make_async_copy(src, dst, arecv.at[p])

    def to_plane(p):
        for xd in range(4):
            for half in range(2):
                z_copy(p, xd, half, STEPS - 1).wait_recv()
            zsum[p, xd] = (pbuf[p, xd] + recvbuf[p, xd, STEPS - 1].astype(F32)).astype(BF16)

        @pl.loop(0, 16)
        def _(i):
            mine, remote, local = plane_copy(p, i)

            @pl.when(mine)
            def _():
                local.start()

            @pl.when(jnp.logical_not(mine))
            def _():
                remote.start()

    def span(p):
        return slice(0, 256) if p == 0 else slice(256, 640)

    def code_copy(p, i):
        zd, yhd = lax.div(i, 2), lax.rem(i, 2)
        ref = cg.at[z, yh, c, :, span(p)]
        mine = (zd == z) & (yhd == yh)
        skip = mine if p == 1 else mine | (yhd != yh)
        return skip, pltpu.make_async_remote_copy(
            ref, ref, gsend.at[p], grecv.at[p], device(zd, yhd * 2 + yl, x, c), MESH
        )

    def over_y():
        ref = cg.at[:, yh, c, :, span(0)]
        to = device(z, (1 - yh) * 2 + yl, x, c)
        return pltpu.make_async_remote_copy(ref, ref, ysend, yrecv, to, MESH)

    def update(p):
        pltpu.make_async_copy(a2a.at[p], a2a.at[p], arecv.at[p]).wait()
        total = a2a[p, 0].astype(F32)
        for i in range(1, 16):
            total = total + a2a[p, i].astype(F32)
        cols = slice(p * 256, (p + 1) * 256)
        gradient = total / 256.0
        moment_new = FIRST_DECAY * moment[:, cols] + (1.0 - FIRST_DECAY) * gradient
        second_new = SECOND_DECAY * second[:, cols] + (1.0 - SECOND_DECAY) * gradient * gradient
        step_size = moment_new / FIRST_FIX / (jnp.sqrt(second_new / SECOND_FIX) + ADAM_EPSILON)
        master_new = master[:, cols] - LEARN_RATE * step_size
        grad_out[:, cols] = gradient
        moment_out[:, cols] = moment_new
        second_out[:, cols] = second_new
        master_out[:, cols] = master_new
        peak = jnp.max(jnp.abs(master_new), axis=1, keepdims=True)
        scale = ((peak + SCALE_EPSILON) / CODE_RANGE).astype(BF16).astype(F32)
        cg[z, yh, c, :, cols] = (master_new / scale).astype(BF16)
        spread = jnp.broadcast_to(scale, (32, HEAD))
        if p == 1:
            at = lax.broadcasted_iota(jnp.int32, (32, HEAD), 1)
            spread = jnp.where(at == 0, cg[z, yh, c, :, 512:640].astype(F32), spread)
        cg[z, yh, c, :, 512:640] = spread.astype(BF16)

        @pl.loop(0, 16)
        def _(i):
            mine, remote = code_copy(p, i)

            @pl.when(jnp.logical_not(mine))
            def _():
                remote.start()

    def arrived(p, sem):
        same = cg.at[pl.ds(0, 7), 0, 0, :, span(0)] if p == 0 else hid.at[0:32, 0 : 15 * 384]
        pltpu.make_async_copy(same, same, sem).wait()

    def put(p, core):
        ref = cg.at[:, :, core, :, span(p)]
        return pltpu.make_async_copy(ref, cg_hbm.at[:, :, core, :, span(p)], cg_sem)

    def pass_copy(p):
        ref = cg.at[:, :, c, :, span(p)]
        return pltpu.make_async_remote_copy(
            ref, ref, dsend.at[p], drecv.at[p], partner, MESH
        )

    for xd in range(4):
        send_hidden(xd).wait_recv()
    send_back.wait_recv()
    partials(0, 0)

    @pl.loop(0, STEPS + LAG)
    def _(t):
        @pl.when(t < STEPS)
        def _():
            z_step(0, t)

        @pl.when(t == LAG - 1)
        def _():
            partials(1, 0)

        @pl.when(t >= LAG)
        def _():
            z_step(1, t - LAG)

        @pl.when(t == 1)
        def _():
            use_block(x, yl, True)

        @pl.when(t == 2)
        def _():
            w_wait(xs[-1], yl, c, 0)
            to_x(xs[-1], 0, 1)
            to_y(xs[-1], 0)
            to_partner(xs[-1], yl, 0)
            w_wait(xs[1], yl, c, 0)
            to_y(xs[1], 0)
            to_partner(xs[1], yl, 0)
            for q in range(2):
                w_wait(x, 1 - yl, c, q)
                to_partner(x, 1 - yl, q)

        @pl.when(t == 3)
        def _():
            w_wait(xs[1], yl, c, 1)
            to_x(xs[1], 1, -1)
            to_y(xs[1], 1)
            to_partner(xs[1], yl, 1)
            w_wait(xs[-1], yl, c, 1)
            to_y(xs[-1], 1)
            to_partner(xs[-1], yl, 1)
            use_block(x, 1 - yl)

        @pl.when(t == 4)
        def _():
            for d in (-1, 1):
                use_block(xs[d], yl)

        @pl.when(t == 5)
        def _():
            for q in range(2):
                w_wait(xs[2], yl, c, q)
                to_y(xs[2], q)
                to_partner(xs[2], yl, q)
            for d in (-1, 1):
                w_wait(xs[d], 1 - yl, c, 0)
                to_partner(xs[d], 1 - yl, 0)

        @pl.when(t == 6)
        def _():
            to_plane(0)
            for d in (-1, 1):
                w_wait(xs[d], 1 - yl, c, 1)
                to_partner(xs[d], 1 - yl, 1)
            use_block(xs[2], yl)

        @pl.when(t == 7)
        def _():
            for d in (-1, 1):
                use_block(xs[d], 1 - yl)

        @pl.when(t == 8)
        def _():
            update(0)
            for q in range(2):
                w_wait(xs[2], 1 - yl, c, q)
                to_partner(xs[2], 1 - yl, q)

    to_plane(1)
    arrived(0, grecv.at[0])
    over_y().start()
    use_block(xs[2], 1 - yl)
    for h in range(4):
        s = slice(h * HEAD, (h + 1) * HEAD)
        v = acc[:, s]
        keys_out[:, s] = (v * cos + pltpu.roll(v, HEAD // 2, 1) * sin).astype(BF16)
    outs = [pltpu.make_async_copy(keys_out, keys_hbm, out_sem.at[0])]
    outs[0].start()
    update(1)
    for i, (src, dst) in enumerate((
        (grad_out, grad_hbm), (master_out, master_out_hbm),
        (moment_out, moment_out_hbm), (second_out, second_out_hbm),
    )):
        outs.append(pltpu.make_async_copy(src, dst, out_sem.at[i + 1]))
        outs[-1].start()
    over_y().wait_recv()
    pass_copy(0).start()
    put(0, c).start()
    pass_copy(0).wait_recv()
    put(0, oc).start()
    arrived(1, grecv.at[1])
    pass_copy(1).start()
    put(1, c).start()

    pltpu.make_async_copy(hidp, hidp, hsend).wait()
    send_back.wait_send()
    pltpu.make_async_copy(wg.at[pl.ds(0, 7)], wg.at[pl.ds(0, 7)], wsend).wait()
    pltpu.make_async_copy(sendbuf, sendbuf, zsend).wait()
    for p in range(2):
        @pl.when(yl == c)
        def _():
            part = a2a.at[p, pl.ds(0, 15)]
            pltpu.make_async_copy(part, part, asend.at[p]).wait()

        @pl.when(yl != c)
        def _():
            pltpu.make_async_copy(a2a.at[p], a2a.at[p], asend.at[p]).wait()

        arrived(p, gsend.at[p])
        pass_copy(p).wait_send()
    over_y().wait_send()
    pltpu.make_async_copy(hg, hg_hbm, hg_sem).wait()
    for out in outs:
        out.wait()
    pass_copy(1).wait_recv()
    put(1, oc).start()
    pltpu.make_async_copy(cg, cg_hbm, cg_sem).wait()


def exchange(hidden, key_grad, positions, frequency, codes, scales, master, moment, second):
    vmem = pl.BlockSpec(memory_space=pltpu.VMEM)
    anywhere = pl.BlockSpec(memory_space=pl.ANY)
    hbm = pl.BlockSpec(memory_space=pltpu.HBM)
    dma = pltpu.SemaphoreType.DMA
    state = jax.ShapeDtypeStruct((32, 512), F32)
    return pl.pallas_call(
        exchange_kernel,
        out_shape=(
            jax.ShapeDtypeStruct((256, 8192), BF16),
            jax.ShapeDtypeStruct((256, 512), BF16),
            state, state, state, state,
            jax.ShapeDtypeStruct((8, 2, 2, 32, 640), BF16),
        ),
        in_specs=[hbm] * 2 + [vmem] * 2 + [hbm, vmem] + [hbm] * 3,
        out_specs=(anywhere,) * 7,
        scratch_shapes=[
            pltpu.VMEM((256, 8192), BF16),
            pltpu.VMEM((4, 256, 1024), BF16),
            pltpu.VMEM((256, 512), BF16),
            pltpu.VMEM((256, 512), BF16),
            pltpu.VMEM((8, 1024, 512), BF16),
            pltpu.VMEM((256, 8192), BF16),
            pltpu.VMEM((2, 4, 128, 256), F32),
            pltpu.VMEM((2, 4, STEPS, 128, 256), BF16),
            pltpu.VMEM((2, 4, STEPS, 128, 256), BF16),
            pltpu.VMEM((2, 4, 128, 256), BF16),
            pltpu.VMEM((2, 16, 32, 256), BF16),
            pltpu.VMEM((8, 2, 2, 32, 640), BF16),
            pltpu.VMEM((256, 512), F32),
            pltpu.VMEM((256, 512), BF16),
            pltpu.VMEM((1024, 512), BF16),
            pltpu.VMEM((256, 512), BF16),
            pltpu.VMEM((7, 32, 512), F32),
            dma((6,)), dma, dma, dma((5,)),
            dma, dma((4,)), dma, dma, dma, dma((8, 2, 2)),
            dma, dma((2, 4, 2, STEPS)),
            dma((2,)), dma((2,)), dma((2,)), dma((2,)), dma, dma, dma((2,)), dma((2,)),
        ],
        compiler_params=pltpu.CompilerParams(
            collective_id=0, has_side_effects=True, vmem_limit_bytes=40 * 1024 * 1024
        ),
    )(hidden, key_grad, positions, frequency, codes, scales, master, moment, second)


def finish_kernel(
    hg, keys, grad, master, moment, second, cg,
    hg_out, keys_out, grad_out, master_out, moment_out, second_out, codes_out, scales_out,
    spread, scales_v, in_sem, out_sem,
):
    load = pltpu.make_async_copy(cg.at[:, pl.ds(512, 128)], spread, in_sem)
    load.start()
    pairs = (
        (hg, hg_out), (cg.at[:, pl.ds(0, 512)], codes_out), (keys, keys_out), (grad, grad_out),
        (master, master_out), (moment, moment_out), (second, second_out),
    )
    stores = [pltpu.make_async_copy(a, b, out_sem.at[i]) for i, (a, b) in enumerate(pairs)]
    for store in stores:
        store.start()
    load.wait()
    scales_v[...] = spread[...].astype(F32).T[0:2, :].astype(BF16)
    stores.append(pltpu.make_async_copy(scales_v, scales_out, out_sem.at[7]))
    stores[-1].start()
    for store in stores:
        store.wait()


def finish(hg, keys, grad, master, moment, second, cg):
    anywhere = pl.BlockSpec(memory_space=pl.ANY)
    hbm = pl.BlockSpec(memory_space=pltpu.HBM)
    state = jax.ShapeDtypeStruct((32, 512), F32)
    return pl.pallas_call(
        finish_kernel,
        out_shape=(
            jax.ShapeDtypeStruct((256, 8192), BF16),
            jax.ShapeDtypeStruct((256, 512), BF16),
            state, state, state, state,
            jax.ShapeDtypeStruct((1024, 512), BF16),
            jax.ShapeDtypeStruct((2, 1024), BF16),
        ),
        in_specs=[anywhere] * 7,
        out_specs=(hbm,) * 8,
        scratch_shapes=[
            pltpu.VMEM((1024, 128), BF16), pltpu.VMEM((2, 1024), BF16),
            pltpu.SemaphoreType.DMA, pltpu.SemaphoreType.DMA((8,)),
        ],
        compiler_params=pltpu.CompilerParams(vmem_limit_bytes=4 * 1024 * 1024),
    )(hg, keys, grad, master, moment, second, cg)


def shards(hidden, key_grad, positions, weight_codes, weight_scales, master, moment, second):
    hidden, key_grad, weight_codes, master, moment, second = (
        pltpu.with_memory_space_constraint(v, pltpu.HBM)
        for v in (hidden, key_grad, weight_codes, master, moment, second)
    )
    half = jnp.arange(HEAD // 2, dtype=F32) * (-2.0 / HEAD)
    frequency = jnp.power(F32(ROPE_BASE), jnp.concatenate([half, half]))[None, :]
    hg, keys, grad, master_out, moment_out, second_out, cg = exchange(
        hidden, key_grad, positions.reshape(2, 128), frequency, weight_codes, weight_scales.T,
        master, moment, second,
    )
    hidden_grad, keys, grad, master_out, moment_out, second_out, codes, scales = finish(
        hg, keys, grad, master_out, moment_out, second_out, cg.reshape(1024, 640)
    )
    return (keys, hidden_grad, grad, master_out, moment_out, second_out, codes, scales.T)


def solution(mesh):
    in_specs = (
        P(("wide", "narrow"), None),
        P(("wide", "narrow"), None),
        P(("wide", "narrow")),
        P("narrow", None),
        P("narrow", None),
        P(("narrow", "wide"), None),
        P(("narrow", "wide"), None),
        P(("narrow", "wide"), None),
    )
    out_specs = (
        P(("wide", "narrow"), None),
        P(("wide", "narrow"), None),
        P(("narrow", "wide"), None),
        P(("narrow", "wide"), None),
        P(("narrow", "wide"), None),
        P(("narrow", "wide"), None),
        P("narrow", None),
        P("narrow", None),
    )
    return jax.shard_map(shards, mesh=mesh, in_specs=in_specs, out_specs=out_specs, check_vma=False)
```

```python
import jax
import jax.numpy as jnp
from jax import lax
from jax.experimental import pallas as pl
from jax.experimental.pallas import tpu as pltpu
from jax.sharding import PartitionSpec as P

HEAD = 128
ROPE_BASE = 1000000.0
LEARN_RATE = 0.002
FIRST_DECAY = 0.9
SECOND_DECAY = 0.95
FIRST_FIX = 0.9999734386011124
SECOND_FIX = 0.994079470779666
ADAM_EPSILON = 1e-08
SCALE_EPSILON = 1e-06
CODE_RANGE = 127.0

MESH = pl.DeviceIdType.MESH
F32 = jnp.float32
BF16 = jnp.bfloat16
ZN = 8
STEPS = ZN - 1
WIDTH = (256, 128)
LAG = 2


def device(z, y, x, core):
    return (z * 4 + lax.div(y, 2) * 2 + core, x * 2 + lax.rem(y, 2))


def dot_rows(a, b):
    return lax.dot_general(a, b, (((0,), (0,)), ((), ())), preferred_element_type=F32)


def exchange_kernel(
    hid_hbm, key_grad_hbm, positions_hbm, frequency, codes_hbm, scales_hbm, master_hbm, moment_hbm,
    second_hbm,
    hg_hbm, keys_hbm, grad_hbm, master_out_hbm, moment_out_hbm, second_out_hbm, cg_hbm, sc_hbm,
    hid, hidp, back_out, backp, wg, hg, pbuf, sendbuf, recvbuf, zsum, a2a, cg, acc,
    key_grad, codes, keys_out, state, positions, scales, bpart, b1, b2src, b2, sc, acc0,
    in_sem, hg_sem, cg_sem, out_sem, hsend, hfirst, hrest, bsend, brecv, wsend, wrecv,
    zsend, zrecv, zrecv1, asend, arecv, gsend, grecv, b1send, b1recv, b2send, b2recv, ssend, srecv, s2send, s2recv, ysend, yrecv, dsend, drecv,
):
    master, moment, second, grad_out, master_out, moment_out, second_out = (
        state.at[i] for i in range(7)
    )
    wide = lax.axis_index("wide")
    narrow = lax.axis_index("narrow")
    z, yh, c = lax.div(wide, 4), lax.rem(lax.div(wide, 2), 2), lax.rem(wide, 2)
    x, yl = lax.div(narrow, 2), lax.rem(narrow, 2)
    y = yh * 2 + yl
    oc = 1 - c
    partner = device(z, y, x, oc)
    xs = {d: lax.rem(x + d + 4, 4) for d in (-1, 1, 2)}
    xs[0] = x
    ys = {d: lax.rem(y + d + 4, 4) for d in (-1, 1)}

    loads = [
        pltpu.make_async_copy(src, dst, in_sem.at[i])
        for i, (src, dst) in enumerate((
            (positions_hbm, positions), (key_grad_hbm, key_grad), (hid_hbm, hid),
            (scales_hbm, scales), (codes_hbm, codes),
            (master_hbm, master), (moment_hbm, moment), (second_hbm, second),
        ))
    ]
    for load in loads:
        load.start()

    barrier = pltpu.get_barrier_semaphore()

    @pl.loop(0, 32)
    def _(i):
        to = device(z, lax.rem(lax.div(i, 2), 4), lax.div(i, 8), lax.rem(i, 2))

        @pl.when((to[0] != wide) | (to[1] != narrow))
        def _():
            pl.semaphore_signal(barrier, inc=1, device_id=to, device_id_type=MESH)

    @pl.loop(0, 16)
    def _(i):
        @pl.when(lax.div(i, 2) != z)
        def _():
            to = device(lax.div(i, 2), lax.rem(i, 2) * 2 + yl, x, c)
            pl.semaphore_signal(barrier, inc=1, device_id=to, device_id_type=MESH)

    def way_of(xd):
        return 1 if xd < 2 else -1

    def send_hidden(xd, i):
        at = lax.rem(z + way_of(xd) * (i - 1) + 2 * ZN, ZN)
        src = pl.ds(pl.multiple_of((xd * 2 + oc) * 1024 + at * 128, 128), 128)
        dst = pl.ds(pl.multiple_of(at * 128, 128), 128)
        sem = hfirst.at[xd] if isinstance(i, int) else hrest.at[xd]
        return pltpu.make_async_remote_copy(
            hid.at[:, src], hidp.at[xd, :, dst], hsend, sem, partner, MESH
        )

    loads[0].wait()
    place = jnp.concatenate(
        [jnp.broadcast_to(positions[i : i + 1, :].astype(F32), (128, 128)).T for i in range(2)], 0
    )
    angle = place * frequency[...]
    cos = jnp.cos(angle)
    sin = jnp.sin(angle)
    lane = lax.broadcasted_iota(jnp.int32, (256, HEAD), 1)
    sin = jnp.where(lane < HEAD // 2, -sin, sin)
    loads[1].wait()
    for h in range(4):
        s = slice(h * HEAD, (h + 1) * HEAD)
        v = key_grad[:, s].astype(F32)
        back_out[:, s] = (v * cos - pltpu.roll(v, HEAD // 2, 1) * sin).astype(BF16)
    send_back = pltpu.make_async_remote_copy(back_out, backp, bsend, brecv, partner, MESH)

    def chunk(xb, lo, half, q):
        return wg.at[xb * 2 + lo, pl.ds(pl.multiple_of(half * 512 + q * 256, 256), 256)]

    def w_copy(xb, lo, half, q, target):
        ref = chunk(xb, lo, half, q)
        sem = wrecv.at[xb * 2 + lo, half, q]
        return pltpu.make_async_remote_copy(ref, ref, wsend, sem, target, MESH)

    def w_wait(xb, lo, half, q):
        w_copy(xb, lo, half, q, partner).wait_recv()

    def to_x(xb, q, d):
        w_copy(xb, yl, c, q, device(z, y, xs[d], c)).start()

    def to_y(xb, q):
        w_copy(xb, yl, c, q, device(z, ys[1 - 2 * q], x, c)).start()

    def to_partner(xb, lo, q):
        w_copy(xb, lo, c, q, partner).start()

    pl.semaphore_wait(barrier, 45)
    loads[2].wait()
    for xd in range(4):
        send_hidden(xd, 0).start()
    send_back.start()

    @pl.loop(1, ZN)
    def _(i):
        for xd in range(4):
            send_hidden(xd, i).start()

    pick = (
        lax.broadcasted_iota(jnp.int32, (2, 512), 1) // 256
        == lax.broadcasted_iota(jnp.int32, (2, 512), 0)
    ).astype(BF16)

    loads[3].wait()
    loads[4].wait()

    @pl.loop(0, 8)
    def _(i):
        rows = pl.ds(pl.multiple_of(i * 128, 128), 128)
        factor = dot_rows(scales[:, rows], pick)
        wg[narrow, rows, :] = (codes[rows, :].astype(F32) * factor).astype(BF16)
    for q in range(2):
        to_x(x, q, 1)
        to_x(x, q, -1)
        to_y(x, q)

    def hg_copy(block):
        cols = pl.ds(pl.multiple_of(block * 1024, 1024), 1024)
        return pltpu.make_async_copy(hg.at[:, cols], hg_hbm.at[:, cols], hg_sem)

    def use_block(xb, lo, first=False):
        block = xb * 2 + lo
        if first:
            acc[...] = jnp.zeros_like(acc)
        else:
            w_wait(xb, lo, oc, 0)
            w_wait(xb, lo, oc, 1)

        @pl.loop(0, 4)
        def _(i):
            cols = pl.ds(pl.multiple_of(block * 1024 + i * 256, 256), 256)
            w = wg[block, pl.ds(pl.multiple_of(i * 256, 256), 256), :]
            acc[...] += jnp.dot(hid[:, cols], w, preferred_element_type=F32)
            hg[:, cols] = lax.dot_general(
                back_out[...], w, (((1,), (1,)), ((), ())), preferred_element_type=F32
            ).astype(BF16)

        hg_copy(block).start()

    def partial(xd, at, cols):
        own = pl.ds(pl.multiple_of((xd * 2 + c) * 1024 + at * 128, 128), 128)
        other = pl.ds(pl.multiple_of(at * 128, 128), 128)
        return dot_rows(hid[:, own], back_out[:, cols]) + dot_rows(
            hidp[xd, :, other], backp[:, cols]
        )

    def partials(p, step):
        for xd in range(4):
            at = lax.rem(z - way_of(xd) * (step + 1) + 2 * ZN, ZN)
            cols = slice(p * 256, p * 256 + WIDTH[p])
            pbuf[p, xd, :, 0 : WIDTH[p]] = partial(xd, at, cols)

    def part_rows(p, half):
        return slice(half * 64, half * 64 + 64) if p == 0 else slice(0, 128)

    def z_copy(p, xd, half, step):
        to = device(lax.rem(z + way_of(xd) + ZN, ZN), y, x, c)
        rows, cols = part_rows(p, half), slice(0, WIDTH[p])
        sem = zrecv.at[xd, half, step] if p == 0 else zrecv1.at[xd, step]
        return pltpu.make_async_remote_copy(
            sendbuf.at[p, xd, step, rows, cols], recvbuf.at[p, xd, step, rows, cols],
            zsend.at[p], sem, to, MESH,
        )

    def z_step(p, step):
        cols = slice(0, WIDTH[p])
        for half in range(2 - p):
            rows = part_rows(p, half)
            for xd in (0, 2, 1, 3):
                @pl.when(step > 0)
                def _():
                    z_copy(p, xd, half, step - 1).wait_recv()
                    pbuf[p, xd, rows, cols] += recvbuf[p, xd, step - 1, rows, cols].astype(F32)

                sendbuf[p, xd, step, rows, cols] = pbuf[p, xd, rows, cols].astype(BF16)
                z_copy(p, xd, half, step).start()
        if p == 0:
            @pl.when(step == 0)
            def _():
                for xd in range(4):
                    rest = hidp.at[xd, :, 0 : 7 * 128]
                    pltpu.make_async_copy(rest, rest, hrest.at[xd]).wait()

        partials(p, step + 1)

    def target(i):
        xd, yhd, cd = lax.div(i, 4), lax.rem(lax.div(i, 2), 2), lax.rem(i, 2)
        mine = (xd == x) & (yl == c) & (yhd == yh) & (cd == c)
        rows = pl.ds(pl.multiple_of(yhd * 64 + cd * 32, 32), 32)
        return xd, rows, mine, device(z, yhd * 2 + c, xd, cd)

    def send_plane(i, source, dst, send, recv):
        xd, rows, mine, to = target(i)
        src = source(xd, rows)

        @pl.when(mine)
        def _():
            pltpu.make_async_copy(src, dst, recv).start()

        @pl.when(jnp.logical_not(mine))
        def _():
            pltpu.make_async_remote_copy(src, dst, send, recv, to, MESH).start()

    def sent_plane(ref, send):
        @pl.when(yl == c)
        def _():
            part = ref.at[pl.ds(0, 15)]
            pltpu.make_async_copy(part, part, send).wait()

        @pl.when(yl != c)
        def _():
            pltpu.make_async_copy(ref, ref, send).wait()

    def to_plane(p):
        cols = slice(0, WIDTH[p])
        for xd in range(4):
            for half in range(2 - p):
                z_copy(p, xd, half, STEPS - 1).wait_recv()
            zsum[p, xd, :, cols] = (
                pbuf[p, xd, :, cols] + recvbuf[p, xd, STEPS - 1, :, cols].astype(F32)
            ).astype(BF16)

        @pl.loop(0, 16)
        def _(i):
            send_plane(
                i, lambda xd, rows: zsum.at[p, xd, rows, cols],
                a2a.at[p, x * 4 + y, :, cols], asend.at[p], arecv.at[p],
            )

    def plane_first(xd):
        for k in range(2):
            own = pl.ds(pl.multiple_of((xd * 2 + c) * 1024 + k * 512, 512), 512)
            other = slice(k * 512, k * 512 + 512)
            term = dot_rows(hid[:, own], back_out[:, 384:512]) + dot_rows(
                hidp[xd, :, other], backp[:, 384:512]
            )
            bpart[xd, k * 4 : k * 4 + 4] = term.astype(BF16).reshape(4, 128, 128)

        @pl.loop(xd * 4, xd * 4 + 4)
        def _(i):
            send_plane(
                i, lambda xd, rows: bpart.at[xd, :, rows], b1.at[x * 4 + y], b1send, b1recv
            )

    def then_z(i):
        return pltpu.make_async_remote_copy(
            b2src.at[i], b2.at[z], b2send, b2recv, device(i, y, x, c), MESH
        )

    def plane_done():
        pltpu.make_async_copy(b1, b1, b1recv).wait()

        @pl.loop(0, ZN)
        def _(i):
            total = b1[0, i].astype(F32)
            for k in range(1, 16):
                total = total + b1[k, i].astype(F32)
            b2src[i] = total.astype(BF16)

            @pl.when(i != z)
            def _():
                then_z(i).start()

        b2[z] = b2src[z]

    def span(p):
        return slice(p * 256, p * 256 + 256)

    def code_copy(p, i):
        zd, yhd = lax.div(i, 2), lax.rem(i, 2)
        ref = cg.at[z, yh, c, :, span(p)]
        mine = (zd == z) & (yhd == yh)
        skip = mine if p == 1 else mine | (yhd != yh)
        return skip, pltpu.make_async_remote_copy(
            ref, ref, gsend.at[p], grecv.at[p], device(zd, yhd * 2 + yl, x, c), MESH
        )

    def scale_copy(i):
        ref = sc.at[z, yh, c]
        to = device(lax.div(i, 2), lax.rem(i, 2) * 2 + yl, x, c)
        return pltpu.make_async_remote_copy(ref, ref, ssend, srecv, to, MESH)

    def over_y():
        ref = cg.at[:, yh, c, :, span(0)]
        to = device(z, (1 - yh) * 2 + yl, x, c)
        return pltpu.make_async_remote_copy(ref, ref, ysend, yrecv, to, MESH)

    def update(p):
        came = a2a.at[p, :, :, 0 : WIDTH[p]]
        pltpu.make_async_copy(came, came, arecv.at[p]).wait()
        total = a2a[p, 0, :, 0 : WIDTH[p]].astype(F32)
        for i in range(1, 16):
            total = total + a2a[p, i, :, 0 : WIDTH[p]].astype(F32)
        if p == 1:
            most = b2.at[pl.ds(0, 7)]
            pltpu.make_async_copy(most, most, b2recv).wait()
            rest = b2[0].astype(F32)
            for i in range(1, ZN):
                rest = rest + b2[i].astype(F32)
            total = jnp.concatenate([total, rest], 1)
        cols = slice(p * 256, (p + 1) * 256)
        gradient = total / 256.0
        moment_new = FIRST_DECAY * moment[:, cols] + (1.0 - FIRST_DECAY) * gradient
        second_new = SECOND_DECAY * second[:, cols] + (1.0 - SECOND_DECAY) * gradient * gradient
        step_size = moment_new / FIRST_FIX / (jnp.sqrt(second_new / SECOND_FIX) + ADAM_EPSILON)
        master_new = master[:, cols] - LEARN_RATE * step_size
        grad_out[:, cols] = gradient
        moment_out[:, cols] = moment_new
        second_out[:, cols] = second_new
        master_out[:, cols] = master_new
        peak = jnp.max(jnp.abs(master_new), axis=1, keepdims=True)
        scale = ((peak + SCALE_EPSILON) / CODE_RANGE).astype(BF16).astype(F32)
        cg[z, yh, c, :, cols] = (master_new / scale).astype(BF16)
        spread = jnp.broadcast_to(scale, (32, HEAD))
        if p == 0:
            acc0[...] = spread
        else:
            at = lax.broadcasted_iota(jnp.int32, (32, HEAD), 1)
            spread = jnp.where(at == 0, acc0[...], spread)
            turned = jnp.concatenate([spread] * 4, 0).T
            group = lax.broadcasted_iota(jnp.int32, (16, HEAD), 1) // 32
            sc[z, yh, c] = jnp.where(group == yh * 2 + c, turned[0:16], 0.0).astype(BF16)

        @pl.loop(0, 16)
        def _(i):
            skip, remote = code_copy(p, i)

            @pl.when(jnp.logical_not(skip))
            def _():
                remote.start()
                if p == 1:
                    scale_copy(i).start()

    def arrived(p, sem):
        same = cg.at[pl.ds(0, 7), 0, 0, :, span(0)] if p == 0 else a2a.at[0, pl.ds(0, 15)]
        pltpu.make_async_copy(same, same, sem).wait()

    def scales_arrived(sem):
        same = b1.at[0:15, 0, 0:16]
        pltpu.make_async_copy(same, same, sem).wait()

    def pass_scales():
        ref = sc.at[:, :, c]
        return pltpu.make_async_remote_copy(ref, ref, s2send, s2recv, partner, MESH)

    def put(p, core):
        ref = cg.at[:, :, core, :, span(p)]
        return pltpu.make_async_copy(ref, cg_hbm.at[:, :, core, :, span(p)], cg_sem)

    def pass_copy(p):
        ref = cg.at[:, :, c, :, span(p)]
        return pltpu.make_async_remote_copy(
            ref, ref, dsend.at[p], drecv.at[p], partner, MESH
        )

    for xd in range(4):
        send_hidden(xd, 0).wait_recv()
    send_back.wait_recv()
    partials(0, 0)

    @pl.loop(0, STEPS + LAG)
    def _(t):
        @pl.when(t < STEPS)
        def _():
            z_step(0, t)

        @pl.when(t == LAG - 1)
        def _():
            partials(1, 0)

        @pl.when(t >= LAG)
        def _():
            z_step(1, t - LAG)

        for k in range(4):
            @pl.when(t == k)
            def _():
                plane_first(k)

        @pl.when(t == 2)
        def _():
            w_wait(xs[-1], yl, c, 0)
            to_x(xs[-1], 0, 1)
            to_y(xs[-1], 0)
            to_partner(xs[-1], yl, 0)
            w_wait(xs[1], yl, c, 0)
            to_y(xs[1], 0)
            to_partner(xs[1], yl, 0)
            for q in range(2):
                w_wait(x, 1 - yl, c, q)
                to_partner(x, 1 - yl, q)
            use_block(x, yl, True)

        @pl.when(t == 4)
        def _():
            w_wait(xs[1], yl, c, 1)
            to_x(xs[1], 1, -1)
            to_y(xs[1], 1)
            to_partner(xs[1], yl, 1)
            w_wait(xs[-1], yl, c, 1)
            to_y(xs[-1], 1)
            to_partner(xs[-1], yl, 1)
            use_block(x, 1 - yl)

        @pl.when(t == 5)
        def _():
            for d in (-1, 1):
                use_block(xs[d], yl)

        @pl.when(t == 7)
        def _():
            to_plane(0)
            plane_done()

        @pl.when(t == 8)
        def _():
            for q in range(2):
                w_wait(xs[2], yl, c, q)
                to_y(xs[2], q)
                to_partner(xs[2], yl, q)

    to_plane(1)
    for load in loads[5:]:
        load.wait()
    for d in (-1, 1):
        w_wait(xs[d], 1 - yl, c, 0)
        to_partner(xs[d], 1 - yl, 0)
    use_block(xs[2], yl)
    update(0)
    for d in (-1, 1):
        w_wait(xs[d], 1 - yl, c, 1)
        to_partner(xs[d], 1 - yl, 1)
    for d in (-1, 1):
        use_block(xs[d], 1 - yl)
    update(1)
    arrived(0, grecv.at[0])
    over_y().start()
    outs = []
    for i, (src, dst) in enumerate((
        (grad_out, grad_hbm), (master_out, master_out_hbm),
        (moment_out, moment_out_hbm), (second_out, second_out_hbm),
    )):
        outs.append(pltpu.make_async_copy(src, dst, out_sem.at[i + 1]))
        outs[-1].start()
    for q in range(2):
        w_wait(xs[2], 1 - yl, c, q)
        to_partner(xs[2], 1 - yl, q)
    over_y().wait_recv()
    pass_copy(0).start()
    put(0, c).start()
    use_block(xs[2], 1 - yl)
    for h in range(4):
        s = slice(h * HEAD, (h + 1) * HEAD)
        v = acc[:, s]
        keys_out[:, s] = (v * cos + pltpu.roll(v, HEAD // 2, 1) * sin).astype(BF16)
    outs.append(pltpu.make_async_copy(keys_out, keys_hbm, out_sem.at[0]))
    outs[-1].start()
    pass_copy(0).wait_recv()
    put(0, oc).start()
    arrived(1, grecv.at[1])
    pass_copy(1).start()
    put(1, c).start()
    scales_arrived(srecv)
    pass_scales().start()

    pltpu.make_async_copy(hidp, hidp, hsend).wait()
    send_back.wait_send()
    pltpu.make_async_copy(wg.at[pl.ds(0, 7)], wg.at[pl.ds(0, 7)], wsend).wait()
    for p in range(2):
        sent = sendbuf.at[p, :, :, :, 0 : WIDTH[p]]
        pltpu.make_async_copy(sent, sent, zsend.at[p]).wait()
        sent_plane(a2a.at[p, :, :, 0 : WIDTH[p]], asend.at[p])
        arrived(p, gsend.at[p])
        pass_copy(p).wait_send()
    over_y().wait_send()
    sent_plane(b1, b1send)
    most = b2.at[pl.ds(0, 7)]
    pltpu.make_async_copy(most, most, b2send).wait()
    scales_arrived(ssend)
    pltpu.make_async_copy(hg, hg_hbm, hg_sem).wait()
    for out in outs:
        out.wait()
    pass_copy(1).wait_recv()
    put(1, oc).start()
    pass_scales().wait()
    last = pltpu.make_async_copy(sc, sc_hbm, out_sem.at[5])
    last.start()
    last.wait()
    pltpu.make_async_copy(cg, cg_hbm, cg_sem).wait()


def exchange(hidden, key_grad, positions, frequency, codes, scales, master, moment, second):
    vmem = pl.BlockSpec(memory_space=pltpu.VMEM)
    anywhere = pl.BlockSpec(memory_space=pl.ANY)
    hbm = pl.BlockSpec(memory_space=pltpu.HBM)
    dma = pltpu.SemaphoreType.DMA
    state = jax.ShapeDtypeStruct((32, 512), F32)
    return pl.pallas_call(
        exchange_kernel,
        out_shape=(
            jax.ShapeDtypeStruct((256, 8192), BF16),
            jax.ShapeDtypeStruct((256, 512), BF16),
            state, state, state, state,
            jax.ShapeDtypeStruct((8, 2, 2, 32, 512), BF16),
            jax.ShapeDtypeStruct((8, 2, 2, 16, 128), BF16),
        ),
        in_specs=[hbm] * 3 + [vmem] + [hbm] * 5,
        out_specs=(anywhere,) * 8,
        scratch_shapes=[
            pltpu.VMEM((256, 8192), BF16),
            pltpu.VMEM((4, 256, 1024), BF16),
            pltpu.VMEM((256, 512), BF16),
            pltpu.VMEM((256, 512), BF16),
            pltpu.VMEM((8, 1024, 512), BF16),
            pltpu.VMEM((256, 8192), BF16),
            pltpu.VMEM((2, 4, 128, 256), F32),
            pltpu.VMEM((2, 4, STEPS, 128, 256), BF16),
            pltpu.VMEM((2, 4, STEPS, 128, 256), BF16),
            pltpu.VMEM((2, 4, 128, 256), BF16),
            pltpu.VMEM((2, 16, 32, 256), BF16),
            pltpu.VMEM((8, 2, 2, 32, 512), BF16),
            pltpu.VMEM((256, 512), F32),
            pltpu.VMEM((256, 512), BF16),
            pltpu.VMEM((1024, 512), BF16),
            pltpu.VMEM((256, 512), BF16),
            pltpu.VMEM((7, 32, 512), F32),
            pltpu.VMEM((2, 128), jnp.int32),
            pltpu.VMEM((2, 1024), BF16),
            pltpu.VMEM((4, 8, 128, 128), BF16),
            pltpu.VMEM((16, 8, 32, 128), BF16),
            pltpu.VMEM((8, 32, 128), BF16),
            pltpu.VMEM((8, 32, 128), BF16),
            pltpu.VMEM((8, 2, 2, 16, 128), BF16),
            pltpu.VMEM((32, 128), F32),
            dma((8,)), dma, dma, dma((6,)),
            dma, dma((4,)), dma((4,)), dma, dma, dma, dma((8, 2, 2)),
            dma((2,)), dma((4, 2, STEPS)), dma((4, STEPS)),
            dma((2,)), dma((2,)), dma((2,)), dma((2,)),
            dma, dma, dma, dma, dma, dma, dma, dma,
            dma, dma, dma((2,)), dma((2,)),
        ],
        compiler_params=pltpu.CompilerParams(
            collective_id=0, has_side_effects=True, vmem_limit_bytes=44 * 1024 * 1024
        ),
    )(hidden, key_grad, positions, frequency, codes, scales, master, moment, second)


def finish_kernel(
    hg, keys, grad, master, moment, second, cg, sc,
    hg_out, keys_out, grad_out, master_out, moment_out, second_out, codes_out, scales_out,
    spread, scales_v, in_sem, out_sem,
):
    load = pltpu.make_async_copy(sc, spread, in_sem)
    load.start()
    pairs = (
        *((hg.at[pl.ds(64 * i, 64)], hg_out.at[pl.ds(64 * i, 64)]) for i in range(4)),
        (cg, codes_out), (keys, keys_out), (grad, grad_out),
        (master, master_out), (moment, moment_out), (second, second_out),
    )
    stores = [pltpu.make_async_copy(a, b, out_sem.at[i]) for i, (a, b) in enumerate(pairs)]
    for store in stores:
        store.start()
    load.wait()
    for i in range(8):
        total = spread[4 * i].astype(F32)
        for k in range(1, 4):
            total = total + spread[4 * i + k].astype(F32)
        scales_v[:, i * 128 : (i + 1) * 128] = total[0:2, :].astype(BF16)
    stores.append(pltpu.make_async_copy(scales_v, scales_out, out_sem.at[10]))
    stores[-1].start()
    for store in stores:
        store.wait()


def finish(hg, keys, grad, master, moment, second, cg, sc):
    anywhere = pl.BlockSpec(memory_space=pl.ANY)
    hbm = pl.BlockSpec(memory_space=pltpu.HBM)
    state = jax.ShapeDtypeStruct((32, 512), F32)
    return pl.pallas_call(
        finish_kernel,
        out_shape=(
            jax.ShapeDtypeStruct((256, 8192), BF16),
            jax.ShapeDtypeStruct((256, 512), BF16),
            state, state, state, state,
            jax.ShapeDtypeStruct((1024, 512), BF16),
            jax.ShapeDtypeStruct((2, 1024), BF16),
        ),
        in_specs=[anywhere] * 8,
        out_specs=(hbm,) * 8,
        scratch_shapes=[
            pltpu.VMEM((32, 16, 128), BF16), pltpu.VMEM((2, 1024), BF16),
            pltpu.SemaphoreType.DMA, pltpu.SemaphoreType.DMA((11,)),
        ],
        compiler_params=pltpu.CompilerParams(vmem_limit_bytes=4 * 1024 * 1024),
    )(hg, keys, grad, master, moment, second, cg, sc)


def shards(hidden, key_grad, positions, weight_codes, weight_scales, master, moment, second):
    positions, weight_scales = positions.reshape(2, 128), weight_scales.T
    hidden, key_grad, positions, weight_codes, weight_scales, master, moment, second = (
        pltpu.with_memory_space_constraint(v, pltpu.HBM)
        for v in (
            hidden, key_grad, positions, weight_codes, weight_scales, master, moment, second
        )
    )
    half = jnp.arange(HEAD // 2, dtype=F32) * (-2.0 / HEAD)
    frequency = jnp.power(F32(ROPE_BASE), jnp.concatenate([half, half]))[None, :]
    hg, keys, grad, master_out, moment_out, second_out, cg, sc = exchange(
        hidden, key_grad, positions, frequency, weight_codes, weight_scales,
        master, moment, second,
    )
    hidden_grad, keys, grad, master_out, moment_out, second_out, codes, scales = finish(
        hg, keys, grad, master_out, moment_out, second_out, cg.reshape(1024, 512),
        sc.reshape(32, 16, 128),
    )
    return (keys, hidden_grad, grad, master_out, moment_out, second_out, codes, scales.T)


def solution(mesh):
    in_specs = (
        P(("wide", "narrow"), None),
        P(("wide", "narrow"), None),
        P(("wide", "narrow")),
        P("narrow", None),
        P("narrow", None),
        P(("narrow", "wide"), None),
        P(("narrow", "wide"), None),
        P(("narrow", "wide"), None),
    )
    out_specs = (
        P(("wide", "narrow"), None),
        P(("wide", "narrow"), None),
        P(("narrow", "wide"), None),
        P(("narrow", "wide"), None),
        P(("narrow", "wide"), None),
        P(("narrow", "wide"), None),
        P("narrow", None),
        P("narrow", None),
    )
    return jax.shard_map(shards, mesh=mesh, in_specs=in_specs, out_specs=out_specs, check_vma=False)
```

```python
import jax
import jax.numpy as jnp
from jax import lax
from jax.experimental import pallas as pl
from jax.experimental.pallas import tpu as pltpu
from jax.sharding import PartitionSpec as P

HEAD = 128
ROPE_BASE = 1000000.0
LEARN_RATE = 0.002
FIRST_DECAY = 0.9
SECOND_DECAY = 0.95
FIRST_FIX = 0.9999734386011124
SECOND_FIX = 0.994079470779666
ADAM_EPSILON = 1e-08
SCALE_EPSILON = 1e-06
CODE_RANGE = 127.0

MESH = pl.DeviceIdType.MESH
F32 = jnp.float32
BF16 = jnp.bfloat16
ZN = 8
STEPS = ZN - 1
WIDTH = (256, 128)
LAG = 2


def device(z, y, x, core):
    return (z * 4 + lax.div(y, 2) * 2 + core, x * 2 + lax.rem(y, 2))


def dot_rows(a, b):
    return lax.dot_general(a, b, (((0,), (0,)), ((), ())), preferred_element_type=F32)


def exchange_kernel(
    hid_hbm, key_grad_hbm, positions_hbm, frequency, codes_hbm, scales_hbm, master_hbm, moment_hbm,
    second_hbm,
    hg_hbm, keys_hbm, grad_hbm, master_out_hbm, moment_out_hbm, second_out_hbm, cg_hbm, sc_hbm,
    hid, hidp, back_out, backp, wg, hg, pbuf, sendbuf, recvbuf, zsum, a2a, cg, acc,
    key_grad, codes, keys_out, state, positions, scales, bpart, b1, b2src, b2, sc, acc0,
    in_sem, hg_sem, cg_sem, out_sem, hsend, hfirst, hrest, bsend, brecv, wsend, wrecv,
    zsend, zrecv, zrecv1, asend, arecv, gsend, grecv, b1send, b1recv, b2send, b2recv, ssend, srecv, s2send, s2recv, ysend, yrecv, dsend, drecv,
):
    master, moment, second, grad_out, master_out, moment_out, second_out = (
        state.at[i] for i in range(7)
    )
    wide = lax.axis_index("wide")
    narrow = lax.axis_index("narrow")
    z, yh, c = lax.div(wide, 4), lax.rem(lax.div(wide, 2), 2), lax.rem(wide, 2)
    x, yl = lax.div(narrow, 2), lax.rem(narrow, 2)
    y = yh * 2 + yl
    oc = 1 - c
    partner = device(z, y, x, oc)
    xs = {d: lax.rem(x + d + 4, 4) for d in (-1, 1, 2)}
    xs[0] = x
    ys = {d: lax.rem(y + d + 4, 4) for d in (-1, 1)}

    loads = [
        pltpu.make_async_copy(src, dst, in_sem.at[i])
        for i, (src, dst) in enumerate((
            (positions_hbm, positions), (key_grad_hbm, key_grad), (hid_hbm, hid),
            (scales_hbm, scales), (codes_hbm, codes),
            (master_hbm, master), (moment_hbm, moment), (second_hbm, second),
        ))
    ]
    for load in loads:
        load.start()

    barrier = pltpu.get_barrier_semaphore()

    @pl.loop(0, 32)
    def _(i):
        to = device(z, lax.rem(lax.div(i, 2), 4), lax.div(i, 8), lax.rem(i, 2))

        @pl.when((to[0] != wide) | (to[1] != narrow))
        def _():
            pl.semaphore_signal(barrier, inc=1, device_id=to, device_id_type=MESH)

    @pl.loop(0, 16)
    def _(i):
        @pl.when(lax.div(i, 2) != z)
        def _():
            to = device(lax.div(i, 2), lax.rem(i, 2) * 2 + yl, x, c)
            pl.semaphore_signal(barrier, inc=1, device_id=to, device_id_type=MESH)

    def way_of(xd):
        return 1 if xd < 2 else -1

    def send_hidden(xd, i):
        at = lax.rem(z + way_of(xd) * (i - 1) + 2 * ZN, ZN)
        src = pl.ds(pl.multiple_of((xd * 2 + oc) * 1024 + at * 128, 128), 128)
        dst = pl.ds(pl.multiple_of(at * 128, 128), 128)
        sem = hfirst.at[xd] if isinstance(i, int) else hrest.at[xd]
        return pltpu.make_async_remote_copy(
            hid.at[:, src], hidp.at[xd, :, dst], hsend, sem, partner, MESH
        )

    loads[0].wait()
    place = jnp.concatenate(
        [jnp.broadcast_to(positions[i : i + 1, :].astype(F32), (128, 128)).T for i in range(2)], 0
    )
    angle = place * frequency[...]
    cos = jnp.cos(angle)
    sin = jnp.sin(angle)
    lane = lax.broadcasted_iota(jnp.int32, (256, HEAD), 1)
    sin = jnp.where(lane < HEAD // 2, -sin, sin)
    loads[1].wait()
    for h in range(4):
        s = slice(h * HEAD, (h + 1) * HEAD)
        v = key_grad[:, s].astype(F32)
        back_out[:, s] = (v * cos - pltpu.roll(v, HEAD // 2, 1) * sin).astype(BF16)
    send_back = pltpu.make_async_remote_copy(back_out, backp, bsend, brecv, partner, MESH)

    def chunk(xb, lo, half, q):
        return wg.at[xb * 2 + lo, pl.ds(pl.multiple_of(half * 512 + q * 256, 256), 256)]

    def w_copy(xb, lo, half, q, target):
        ref = chunk(xb, lo, half, q)
        sem = wrecv.at[xb * 2 + lo, half, q]
        return pltpu.make_async_remote_copy(ref, ref, wsend, sem, target, MESH)

    def w_wait(xb, lo, half, q):
        w_copy(xb, lo, half, q, partner).wait_recv()

    def to_x(xb, q, d):
        w_copy(xb, yl, c, q, device(z, y, xs[d], c)).start()

    def to_y(xb, q):
        w_copy(xb, yl, c, q, device(z, ys[1 - 2 * q], x, c)).start()

    def to_partner(xb, lo, q):
        w_copy(xb, lo, c, q, partner).start()

    pl.semaphore_wait(barrier, 45)
    loads[2].wait()
    for xd in range(4):
        send_hidden(xd, 0).start()
    send_back.start()

    @pl.loop(1, ZN)
    def _(i):
        for xd in range(4):
            send_hidden(xd, i).start()

    pick = (
        lax.broadcasted_iota(jnp.int32, (2, 512), 1) // 256
        == lax.broadcasted_iota(jnp.int32, (2, 512), 0)
    ).astype(BF16)

    loads[3].wait()
    loads[4].wait()

    @pl.loop(0, 8)
    def _(i):
        rows = pl.ds(pl.multiple_of(i * 128, 128), 128)
        factor = dot_rows(scales[:, rows], pick)
        wg[narrow, rows, :] = (codes[rows, :].astype(F32) * factor).astype(BF16)
    for q in range(2):
        to_x(x, q, 1)
        to_x(x, q, -1)
        to_y(x, q)

    def hg_copy(block):
        cols = pl.ds(pl.multiple_of(block * 1024, 1024), 1024)
        return pltpu.make_async_copy(hg.at[:, cols], hg_hbm.at[:, cols], hg_sem)

    def use_block(xb, lo, first=False):
        block = xb * 2 + lo
        if first:
            acc[...] = jnp.zeros_like(acc)
        else:
            w_wait(xb, lo, oc, 0)
            w_wait(xb, lo, oc, 1)

        @pl.loop(0, 4)
        def _(i):
            cols = pl.ds(pl.multiple_of(block * 1024 + i * 256, 256), 256)
            w = wg[block, pl.ds(pl.multiple_of(i * 256, 256), 256), :]
            acc[...] += jnp.dot(hid[:, cols], w, preferred_element_type=F32)
            hg[:, cols] = lax.dot_general(
                back_out[...], w, (((1,), (1,)), ((), ())), preferred_element_type=F32
            ).astype(BF16)

        hg_copy(block).start()

    def partial(xd, at, cols):
        own = pl.ds(pl.multiple_of((xd * 2 + c) * 1024 + at * 128, 128), 128)
        other = pl.ds(pl.multiple_of(at * 128, 128), 128)
        return dot_rows(hid[:, own], back_out[:, cols]) + dot_rows(
            hidp[xd, :, other], backp[:, cols]
        )

    def partials(p, step):
        for xd in range(4):
            at = lax.rem(z - way_of(xd) * (step + 1) + 2 * ZN, ZN)
            cols = slice(p * 256, p * 256 + WIDTH[p])
            pbuf[p, xd, :, 0 : WIDTH[p]] = partial(xd, at, cols)

    def part_rows(p, half):
        return slice(half * 64, half * 64 + 64) if p == 0 else slice(0, 128)

    def z_copy(p, xd, half, step):
        to = device(lax.rem(z + way_of(xd) + ZN, ZN), y, x, c)
        rows, cols = part_rows(p, half), slice(0, WIDTH[p])
        sem = zrecv.at[xd, half, step] if p == 0 else zrecv1.at[xd, step]
        return pltpu.make_async_remote_copy(
            sendbuf.at[p, xd, step, rows, cols], recvbuf.at[p, xd, step, rows, cols],
            zsend.at[p], sem, to, MESH,
        )

    def z_step(p, step):
        cols = slice(0, WIDTH[p])
        for half in range(2 - p):
            rows = part_rows(p, half)
            for xd in (0, 2, 1, 3):
                @pl.when(step > 0)
                def _():
                    z_copy(p, xd, half, step - 1).wait_recv()
                    pbuf[p, xd, rows, cols] += recvbuf[p, xd, step - 1, rows, cols].astype(F32)

                sendbuf[p, xd, step, rows, cols] = pbuf[p, xd, rows, cols].astype(BF16)
                z_copy(p, xd, half, step).start()
        if p == 0:
            @pl.when(step == 0)
            def _():
                for xd in range(4):
                    rest = hidp.at[xd, :, 0 : 7 * 128]
                    pltpu.make_async_copy(rest, rest, hrest.at[xd]).wait()

        partials(p, step + 1)

    def target(i):
        xd, yhd, cd = lax.div(i, 4), lax.rem(lax.div(i, 2), 2), lax.rem(i, 2)
        mine = (xd == x) & (yl == c) & (yhd == yh) & (cd == c)
        rows = pl.ds(pl.multiple_of(yhd * 64 + cd * 32, 32), 32)
        return xd, rows, mine, device(z, yhd * 2 + c, xd, cd)

    def send_plane(i, source, dst, send, recv):
        xd, rows, mine, to = target(i)
        src = source(xd, rows)

        @pl.when(mine)
        def _():
            pltpu.make_async_copy(src, dst, recv).start()

        @pl.when(jnp.logical_not(mine))
        def _():
            pltpu.make_async_remote_copy(src, dst, send, recv, to, MESH).start()

    def sent_plane(ref, send):
        @pl.when(yl == c)
        def _():
            part = ref.at[pl.ds(0, 15)]
            pltpu.make_async_copy(part, part, send).wait()

        @pl.when(yl != c)
        def _():
            pltpu.make_async_copy(ref, ref, send).wait()

    def to_plane(p):
        cols = slice(0, WIDTH[p])
        for xd in range(4):
            for half in range(2 - p):
                z_copy(p, xd, half, STEPS - 1).wait_recv()
            zsum[p, xd, :, cols] = (
                pbuf[p, xd, :, cols] + recvbuf[p, xd, STEPS - 1, :, cols].astype(F32)
            ).astype(BF16)

        @pl.loop(0, 16)
        def _(i):
            send_plane(
                i, lambda xd, rows: zsum.at[p, xd, rows, cols],
                a2a.at[p, x * 4 + y, :, cols], asend.at[p], arecv.at[p],
            )

    def plane_first(xd):
        for k in range(2):
            own = pl.ds(pl.multiple_of((xd * 2 + c) * 1024 + k * 512, 512), 512)
            other = slice(k * 512, k * 512 + 512)
            term = dot_rows(hid[:, own], back_out[:, 384:512]) + dot_rows(
                hidp[xd, :, other], backp[:, 384:512]
            )
            bpart[xd, k * 4 : k * 4 + 4] = term.astype(BF16).reshape(4, 128, 128)

        @pl.loop(xd * 4, xd * 4 + 4)
        def _(i):
            send_plane(
                i, lambda xd, rows: bpart.at[xd, :, rows], b1.at[x * 4 + y], b1send, b1recv
            )

    def then_z(i):
        return pltpu.make_async_remote_copy(
            b2src.at[i], b2.at[z], b2send, b2recv, device(i, y, x, c), MESH
        )

    def plane_done():
        pltpu.make_async_copy(b1, b1, b1recv).wait()

        @pl.loop(0, ZN)
        def _(i):
            total = b1[0, i].astype(F32)
            for k in range(1, 16):
                total = total + b1[k, i].astype(F32)
            b2src[i] = total.astype(BF16)

            @pl.when(i != z)
            def _():
                then_z(i).start()

        b2[z] = b2src[z]

    def span(p):
        return slice(p * 256, p * 256 + 256)

    def code_copy(p, i):
        zd, yhd = lax.div(i, 2), lax.rem(i, 2)
        ref = cg.at[z, yh, c, :, span(p)]
        mine = (zd == z) & (yhd == yh)
        skip = mine if p == 1 else mine | (yhd != yh)
        return skip, pltpu.make_async_remote_copy(
            ref, ref, gsend.at[p], grecv.at[p], device(zd, yhd * 2 + yl, x, c), MESH
        )

    def scale_copy(i):
        ref = sc.at[z, yh, c]
        to = device(lax.div(i, 2), lax.rem(i, 2) * 2 + yl, x, c)
        return pltpu.make_async_remote_copy(ref, ref, ssend, srecv, to, MESH)

    def over_y():
        ref = cg.at[:, yh, c, :, span(0)]
        to = device(z, (1 - yh) * 2 + yl, x, c)
        return pltpu.make_async_remote_copy(ref, ref, ysend, yrecv, to, MESH)

    def update(p):
        came = a2a.at[p, :, :, 0 : WIDTH[p]]
        pltpu.make_async_copy(came, came, arecv.at[p]).wait()
        total = a2a[p, 0, :, 0 : WIDTH[p]].astype(F32)
        for i in range(1, 16):
            total = total + a2a[p, i, :, 0 : WIDTH[p]].astype(F32)
        if p == 1:
            most = b2.at[pl.ds(0, 7)]
            pltpu.make_async_copy(most, most, b2recv).wait()
            rest = b2[0].astype(F32)
            for i in range(1, ZN):
                rest = rest + b2[i].astype(F32)
            total = jnp.concatenate([total, rest], 1)
        cols = slice(p * 256, (p + 1) * 256)
        gradient = total / 256.0
        moment_new = FIRST_DECAY * moment[:, cols] + (1.0 - FIRST_DECAY) * gradient
        second_new = SECOND_DECAY * second[:, cols] + (1.0 - SECOND_DECAY) * gradient * gradient
        step_size = moment_new / FIRST_FIX / (jnp.sqrt(second_new / SECOND_FIX) + ADAM_EPSILON)
        master_new = master[:, cols] - LEARN_RATE * step_size
        grad_out[:, cols] = gradient
        moment_out[:, cols] = moment_new
        second_out[:, cols] = second_new
        master_out[:, cols] = master_new
        peak = jnp.max(jnp.abs(master_new), axis=1, keepdims=True)
        scale = ((peak + SCALE_EPSILON) / CODE_RANGE).astype(BF16).astype(F32)
        cg[z, yh, c, :, cols] = (master_new / scale).astype(BF16)
        spread = jnp.broadcast_to(scale, (32, HEAD))
        if p == 0:
            acc0[...] = spread
        else:
            at = lax.broadcasted_iota(jnp.int32, (32, HEAD), 1)
            spread = jnp.where(at == 0, acc0[...], spread)
            turned = jnp.concatenate([spread] * 4, 0).T
            group = lax.broadcasted_iota(jnp.int32, (16, HEAD), 1) // 32
            sc[z, yh, c] = jnp.where(group == yh * 2 + c, turned[0:16], 0.0).astype(BF16)

        @pl.loop(0, 16)
        def _(i):
            skip, remote = code_copy(p, i)

            @pl.when(jnp.logical_not(skip))
            def _():
                remote.start()
                if p == 1:
                    scale_copy(i).start()

    def arrived(p, sem):
        same = cg.at[pl.ds(0, 7), 0, 0, :, span(0)] if p == 0 else a2a.at[0, pl.ds(0, 15)]
        pltpu.make_async_copy(same, same, sem).wait()

    def scales_arrived(sem):
        same = b1.at[0:15, 0, 0:16]
        pltpu.make_async_copy(same, same, sem).wait()

    def pass_scales():
        ref = sc.at[:, :, c]
        return pltpu.make_async_remote_copy(ref, ref, s2send, s2recv, partner, MESH)

    def put(p, core):
        ref = cg.at[:, :, core, :, span(p)]
        return pltpu.make_async_copy(ref, cg_hbm.at[:, :, core, :, span(p)], cg_sem)

    def pass_copy(p):
        ref = cg.at[:, :, c, :, span(p)]
        return pltpu.make_async_remote_copy(
            ref, ref, dsend.at[p], drecv.at[p], partner, MESH
        )

    for xd in range(4):
        send_hidden(xd, 0).wait_recv()
    send_back.wait_recv()
    partials(0, 0)

    @pl.loop(0, STEPS + LAG)
    def _(t):
        @pl.when(t < STEPS)
        def _():
            z_step(0, t)

        @pl.when(t == LAG - 1)
        def _():
            partials(1, 0)

        @pl.when(t >= LAG)
        def _():
            z_step(1, t - LAG)

        for k in range(4):
            @pl.when(t == k)
            def _():
                plane_first(k)

        @pl.when(t == 2)
        def _():
            w_wait(xs[-1], yl, c, 0)
            to_x(xs[-1], 0, 1)
            to_y(xs[-1], 0)
            to_partner(xs[-1], yl, 0)
            w_wait(xs[1], yl, c, 0)
            to_y(xs[1], 0)
            to_partner(xs[1], yl, 0)
            for q in range(2):
                w_wait(x, 1 - yl, c, q)
                to_partner(x, 1 - yl, q)
            use_block(x, yl, True)

        @pl.when(t == 4)
        def _():
            w_wait(xs[1], yl, c, 1)
            to_x(xs[1], 1, -1)
            to_y(xs[1], 1)
            to_partner(xs[1], yl, 1)
            w_wait(xs[-1], yl, c, 1)
            to_y(xs[-1], 1)
            to_partner(xs[-1], yl, 1)
            use_block(x, 1 - yl)

        @pl.when(t == 5)
        def _():
            for d in (-1, 1):
                use_block(xs[d], yl)

        @pl.when(t == 7)
        def _():
            to_plane(0)
            plane_done()

        @pl.when(t == 8)
        def _():
            for q in range(2):
                w_wait(xs[2], yl, c, q)
                to_y(xs[2], q)
                to_partner(xs[2], yl, q)

    to_plane(1)
    for load in loads[5:]:
        load.wait()
    for d in (-1, 1):
        w_wait(xs[d], 1 - yl, c, 0)
        to_partner(xs[d], 1 - yl, 0)
    update(0)
    for d in (-1, 1):
        w_wait(xs[d], 1 - yl, c, 1)
        to_partner(xs[d], 1 - yl, 1)
    update(1)
    arrived(0, grecv.at[0])
    over_y().start()
    outs = []
    for i, (src, dst) in enumerate((
        (grad_out, grad_hbm), (master_out, master_out_hbm),
        (moment_out, moment_out_hbm), (second_out, second_out_hbm),
    )):
        outs.append(pltpu.make_async_copy(src, dst, out_sem.at[i + 1]))
        outs[-1].start()
    use_block(xs[2], yl)
    for d in (-1, 1):
        use_block(xs[d], 1 - yl)
    for q in range(2):
        w_wait(xs[2], 1 - yl, c, q)
        to_partner(xs[2], 1 - yl, q)
    over_y().wait_recv()
    pass_copy(0).start()
    put(0, c).start()
    use_block(xs[2], 1 - yl)
    for h in range(4):
        s = slice(h * HEAD, (h + 1) * HEAD)
        v = acc[:, s]
        keys_out[:, s] = (v * cos + pltpu.roll(v, HEAD // 2, 1) * sin).astype(BF16)
    outs.append(pltpu.make_async_copy(keys_out, keys_hbm, out_sem.at[0]))
    outs[-1].start()
    pass_copy(0).wait_recv()
    put(0, oc).start()
    arrived(1, grecv.at[1])
    pass_copy(1).start()
    put(1, c).start()
    scales_arrived(srecv)
    pass_scales().start()

    pltpu.make_async_copy(hidp, hidp, hsend).wait()
    send_back.wait_send()
    pltpu.make_async_copy(wg.at[pl.ds(0, 7)], wg.at[pl.ds(0, 7)], wsend).wait()
    for p in range(2):
        sent = sendbuf.at[p, :, :, :, 0 : WIDTH[p]]
        pltpu.make_async_copy(sent, sent, zsend.at[p]).wait()
        sent_plane(a2a.at[p, :, :, 0 : WIDTH[p]], asend.at[p])
        arrived(p, gsend.at[p])
        pass_copy(p).wait_send()
    over_y().wait_send()
    sent_plane(b1, b1send)
    most = b2.at[pl.ds(0, 7)]
    pltpu.make_async_copy(most, most, b2send).wait()
    scales_arrived(ssend)
    pltpu.make_async_copy(hg, hg_hbm, hg_sem).wait()
    for out in outs:
        out.wait()
    pass_copy(1).wait_recv()
    put(1, oc).start()
    pass_scales().wait()
    last = pltpu.make_async_copy(sc, sc_hbm, out_sem.at[5])
    last.start()
    last.wait()
    pltpu.make_async_copy(cg, cg_hbm, cg_sem).wait()


def exchange(hidden, key_grad, positions, frequency, codes, scales, master, moment, second):
    vmem = pl.BlockSpec(memory_space=pltpu.VMEM)
    anywhere = pl.BlockSpec(memory_space=pl.ANY)
    hbm = pl.BlockSpec(memory_space=pltpu.HBM)
    dma = pltpu.SemaphoreType.DMA
    state = jax.ShapeDtypeStruct((32, 512), F32)
    return pl.pallas_call(
        exchange_kernel,
        out_shape=(
            jax.ShapeDtypeStruct((256, 8192), BF16),
            jax.ShapeDtypeStruct((256, 512), BF16),
            state, state, state, state,
            jax.ShapeDtypeStruct((8, 2, 2, 32, 512), BF16),
            jax.ShapeDtypeStruct((8, 2, 2, 16, 128), BF16),
        ),
        in_specs=[hbm] * 3 + [vmem] + [hbm] * 5,
        out_specs=(anywhere,) * 8,
        scratch_shapes=[
            pltpu.VMEM((256, 8192), BF16),
            pltpu.VMEM((4, 256, 1024), BF16),
            pltpu.VMEM((256, 512), BF16),
            pltpu.VMEM((256, 512), BF16),
            pltpu.VMEM((8, 1024, 512), BF16),
            pltpu.VMEM((256, 8192), BF16),
            pltpu.VMEM((2, 4, 128, 256), F32),
            pltpu.VMEM((2, 4, STEPS, 128, 256), BF16),
            pltpu.VMEM((2, 4, STEPS, 128, 256), BF16),
            pltpu.VMEM((2, 4, 128, 256), BF16),
            pltpu.VMEM((2, 16, 32, 256), BF16),
            pltpu.VMEM((8, 2, 2, 32, 512), BF16),
            pltpu.VMEM((256, 512), F32),
            pltpu.VMEM((256, 512), BF16),
            pltpu.VMEM((1024, 512), BF16),
            pltpu.VMEM((256, 512), BF16),
            pltpu.VMEM((7, 32, 512), F32),
            pltpu.VMEM((2, 128), jnp.int32),
            pltpu.VMEM((2, 1024), BF16),
            pltpu.VMEM((4, 8, 128, 128), BF16),
            pltpu.VMEM((16, 8, 32, 128), BF16),
            pltpu.VMEM((8, 32, 128), BF16),
            pltpu.VMEM((8, 32, 128), BF16),
            pltpu.VMEM((8, 2, 2, 16, 128), BF16),
            pltpu.VMEM((32, 128), F32),
            dma((8,)), dma, dma, dma((6,)),
            dma, dma((4,)), dma((4,)), dma, dma, dma, dma((8, 2, 2)),
            dma((2,)), dma((4, 2, STEPS)), dma((4, STEPS)),
            dma((2,)), dma((2,)), dma((2,)), dma((2,)),
            dma, dma, dma, dma, dma, dma, dma, dma,
            dma, dma, dma((2,)), dma((2,)),
        ],
        compiler_params=pltpu.CompilerParams(
            collective_id=0, has_side_effects=True, vmem_limit_bytes=44 * 1024 * 1024
        ),
    )(hidden, key_grad, positions, frequency, codes, scales, master, moment, second)


def finish_kernel(
    hg, keys, grad, master, moment, second, cg, sc,
    hg_out, keys_out, grad_out, master_out, moment_out, second_out, codes_out, scales_out,
    spread, scales_v, in_sem, out_sem,
):
    load = pltpu.make_async_copy(sc, spread, in_sem)
    load.start()
    pairs = (
        *((hg.at[pl.ds(64 * i, 64)], hg_out.at[pl.ds(64 * i, 64)]) for i in range(4)),
        (cg, codes_out), (keys, keys_out), (grad, grad_out),
        (master, master_out), (moment, moment_out), (second, second_out),
    )
    stores = [pltpu.make_async_copy(a, b, out_sem.at[i]) for i, (a, b) in enumerate(pairs)]
    for store in stores:
        store.start()
    load.wait()
    for i in range(8):
        total = spread[4 * i].astype(F32)
        for k in range(1, 4):
            total = total + spread[4 * i + k].astype(F32)
        scales_v[:, i * 128 : (i + 1) * 128] = total[0:2, :].astype(BF16)
    stores.append(pltpu.make_async_copy(scales_v, scales_out, out_sem.at[10]))
    stores[-1].start()
    for store in stores:
        store.wait()


def finish(hg, keys, grad, master, moment, second, cg, sc):
    anywhere = pl.BlockSpec(memory_space=pl.ANY)
    hbm = pl.BlockSpec(memory_space=pltpu.HBM)
    state = jax.ShapeDtypeStruct((32, 512), F32)
    return pl.pallas_call(
        finish_kernel,
        out_shape=(
            jax.ShapeDtypeStruct((256, 8192), BF16),
            jax.ShapeDtypeStruct((256, 512), BF16),
            state, state, state, state,
            jax.ShapeDtypeStruct((1024, 512), BF16),
            jax.ShapeDtypeStruct((2, 1024), BF16),
        ),
        in_specs=[anywhere] * 8,
        out_specs=(hbm,) * 8,
        scratch_shapes=[
            pltpu.VMEM((32, 16, 128), BF16), pltpu.VMEM((2, 1024), BF16),
            pltpu.SemaphoreType.DMA, pltpu.SemaphoreType.DMA((11,)),
        ],
        compiler_params=pltpu.CompilerParams(vmem_limit_bytes=4 * 1024 * 1024),
    )(hg, keys, grad, master, moment, second, cg, sc)


def shards(hidden, key_grad, positions, weight_codes, weight_scales, master, moment, second):
    positions, weight_scales = positions.reshape(2, 128), weight_scales.T
    hidden, key_grad, positions, weight_codes, weight_scales, master, moment, second = (
        pltpu.with_memory_space_constraint(v, pltpu.HBM)
        for v in (
            hidden, key_grad, positions, weight_codes, weight_scales, master, moment, second
        )
    )
    half = jnp.arange(HEAD // 2, dtype=F32) * (-2.0 / HEAD)
    frequency = jnp.power(F32(ROPE_BASE), jnp.concatenate([half, half]))[None, :]
    hg, keys, grad, master_out, moment_out, second_out, cg, sc = exchange(
        hidden, key_grad, positions, frequency, weight_codes, weight_scales,
        master, moment, second,
    )
    hidden_grad, keys, grad, master_out, moment_out, second_out, codes, scales = finish(
        hg, keys, grad, master_out, moment_out, second_out, cg.reshape(1024, 512),
        sc.reshape(32, 16, 128),
    )
    return (keys, hidden_grad, grad, master_out, moment_out, second_out, codes, scales.T)


def solution(mesh):
    in_specs = (
        P(("wide", "narrow"), None),
        P(("wide", "narrow"), None),
        P(("wide", "narrow")),
        P("narrow", None),
        P("narrow", None),
        P(("narrow", "wide"), None),
        P(("narrow", "wide"), None),
        P(("narrow", "wide"), None),
    )
    out_specs = (
        P(("wide", "narrow"), None),
        P(("wide", "narrow"), None),
        P(("narrow", "wide"), None),
        P(("narrow", "wide"), None),
        P(("narrow", "wide"), None),
        P(("narrow", "wide"), None),
        P("narrow", None),
        P("narrow", None),
    )
    return jax.shard_map(shards, mesh=mesh, in_specs=in_specs, out_specs=out_specs, check_vma=False)
```
